32 devices in a mesh: member: 2 (over y), lon: 8 (over z, x), lat: 2 (over core).
Axes of the slice: x: 2, y: 2, z: 4, core: 2. Of those that a mesh axis runs over, the one named last changes fastest.
Arguments:
- state_tokens: bfloat16 [8, 24, 96, 768], P('member', 'lat', 'lon'), parts along dimension 0, may hold values from -32 to 32
- land_mask: int32 [24, 96], P('lat', 'lon'), may hold values 0 or 1
- pad_mask: int32 [24], replicated, may hold values from 0 to 1, as said below
- land_embed: float32 [2, 768], replicated, may hold values from -3 to 3
- w_qkv: bfloat16 [768, 1152], replicated, may hold values from -0.21875 to 0.21875
- w_proj: bfloat16 [384, 768], replicated, may hold values from -0.3125 to 0.3125
- proj_bias: float32 [768], replicated, may hold values from -4 to 4
- norm_gain: float32 [768], replicated, may hold values from 0.5 to 1.5
- norm_shift: float32 [768], replicated, may hold values from -1.5 to 1.5
- bias_table: bfloat16 [4, 2, 12, 3312], P('lat'), may hold values from -3.5 to 320
- index_table: int32 [144, 144], replicated, may hold values from 0 to 3311
Outputs:
- result: bfloat16 [8, 24, 96, 768], P('member', 'lat', 'lon'), parts along dimension 0
The draws below stay inside these ranges and needn't reach their ends.
There are 2 independent parts, one for each index of `member`. The reference program is written for one: setup_inputs(seed, part) draws one part's arguments, and reference() takes and returns one part's arrays. A program takes and returns all parts, laid end to end along the dimension named above; an argument that names none is the same for every part. Nothing has to cross between parts.
Inputs may be any that keep to these rules, and one draw needn't show every extreme that they name: pad_mask is 1 on every row except at most the first 2 and the last 2 of the 24 rows, which are 0 where padded; one of the two ends has exactly 2 padding rows.
All inputs are finite; a program needn't handle non-finite values. No bound on the sum of `land_mask` on one device may be relied on, other than what follows from the above.
Results may differ from the reference program's by a relative error of at most 0.0085.
Values may be sent and summed in bfloat16 or wider, within the bound.
A program may use at most 64 MiB of HBM per device.

```python
import jax
import jax.numpy as jnp
from jax import lax

D = 768
HEADS = 12
HEAD_DIM = 32
WIN_Z = 2
WIN_LAT = 6
WIN_LON = 12
LEVELS = 4
WIN_TOK = 144
BIAS_POS = 3312
LAT = 24
LON = 96
LAT_WIN = 4
Z_WIN = 2


def index_helper(key):
    return jax.random.randint(jax.random.fold_in(key, 11), (WIN_TOK, WIN_TOK), 0, BIAS_POS, dtype=jnp.int32)


def draw_index_table(key, part):
    return index_helper(key)


def draw_bias_table(key, part):
    inner_key = jax.random.fold_in(key, 23)
    full_shape = (LAT_WIN, Z_WIN, HEADS, BIAS_POS)
    entries = jnp.clip(jax.random.normal(inner_key, full_shape, jnp.float32), -3.5, 3.5)
    return entries.astype(jnp.bfloat16)


def draw_state_tokens(key, part):
    subkeys = jax.random.split(jax.random.fold_in(key, 5), 3)
    full_shape = (LEVELS, LAT, LON, D)
    normal_part = jnp.clip(jax.random.normal(subkeys[0], full_shape, jnp.float32), -3.5, 3.5)
    row_scale = jnp.exp(jax.random.uniform(subkeys[1], (LEVELS, LAT, LON, 1), jnp.float32, jnp.log(0.3), jnp.log(3.0)))
    column_scale = jnp.exp(jax.random.uniform(subkeys[2], (D,), jnp.float32, jnp.log(0.3), jnp.log(3.0)))
    drawn_values = normal_part * row_scale * column_scale
    return drawn_values.astype(jnp.bfloat16)


def draw_pad_mask(key, part):
    subkeys = jax.random.split(jax.random.fold_in(key, 31), 2)
    other_end = jax.random.randint(subkeys[0], (), 0, 3, dtype=jnp.int32)
    chosen = jax.random.randint(subkeys[1], (), 0, 2, dtype=jnp.int32)
    north_rows = jnp.where(chosen == 0, 2, other_end)
    south_rows = jnp.where(chosen == 0, other_end, 2)
    positions = jnp.arange(LAT, dtype=jnp.int32)
    row_mask = (positions >= north_rows) & (positions < LAT - south_rows)
    return row_mask.astype(jnp.int32)


def place_ends(result, rng, smallest, high):
    spot = [jax.random.randint(jax.random.fold_in(rng, axis), (), 0, length) for axis, length in enumerate(result.shape)]
    main_axis = result.shape.index(max(result.shape))
    neighbour = spot[:main_axis] + [(spot[main_axis] + 1) % result.shape[main_axis]] + spot[main_axis + 1:]
    return result.at[tuple(spot)].set(smallest).at[tuple(neighbour)].set(high)


def scatter_about(own_key, extent, width, bound, held_as=jnp.bfloat16):
    return jnp.clip(width * jax.random.normal(own_key, extent, jnp.float32), -bound, bound).astype(held_as)


def setup_inputs(seed: int = 0, part: int = 0) -> dict:
    seeds = jax.random.split(jax.random.key(seed), 12)
    part_splits = jax.random.split(jax.random.fold_in(seeds[11], part), 12)
    state_tokens = draw_state_tokens(jax.random.fold_in(jax.random.fold_in(seeds[11], part), 71), part)
    land_mask = place_ends((jax.random.randint(seeds[1], (LAT, LON), 0, 3) < 1).astype(jnp.int32), jax.random.fold_in(seeds[1], 1), 0, 1)
    pad_mask = draw_pad_mask(jax.random.fold_in(seeds[11], 71), part)
    land_embed = scatter_about(seeds[3], (2, D), 0.5, 3.0, jnp.float32)
    w_qkv = scatter_about(seeds[4], (D, 3 * HEADS * HEAD_DIM), D ** -0.5, 0.21875)
    w_proj = scatter_about(seeds[5], (HEADS * HEAD_DIM, D), (HEADS * HEAD_DIM) ** -0.5, 0.3125)
    proj_bias = scatter_about(seeds[6], (D,), 1.0, 4.0, jnp.float32)
    norm_gain = jnp.clip(1.0 + 0.1 * jax.random.normal(seeds[7], (D,), jnp.float32), 0.5, 1.5)
    norm_shift = scatter_about(seeds[8], (D,), 0.3, 1.5, jnp.float32)
    bias_table = draw_bias_table(jax.random.fold_in(seeds[11], 71), part)
    index_table = draw_index_table(jax.random.fold_in(seeds[11], 71), part)
    return dict(state_tokens=state_tokens, land_mask=land_mask, pad_mask=pad_mask, land_embed=land_embed, w_qkv=w_qkv, w_proj=w_proj, proj_bias=proj_bias, norm_gain=norm_gain, norm_shift=norm_shift, bias_table=bias_table, index_table=index_table)


norm_epsilon = 1e-05

def region_of(position, length, window):
    half_window = window // 2
    return jnp.where(position < length - window, 0, jnp.where(position < length - half_window, 1, 2)).astype(jnp.int32)

def window_rules(levels, lat_start, lat_rows, lat_total, pad_mask):
    tokens = jnp.arange(WIN_TOK, dtype=jnp.int32)
    level_offset = tokens // (WIN_LAT * WIN_LON)
    row_offset = tokens // WIN_LON % WIN_LAT
    level_index = jnp.arange(levels // WIN_Z, dtype=jnp.int32)[:, None] * WIN_Z + level_offset[None, :]
    row_index = lat_start + jnp.arange(lat_rows // WIN_LAT, dtype=jnp.int32)[:, None] * WIN_LAT + row_offset[None, :]
    region = region_of(level_index, levels, WIN_Z)[:, None, :] * 3 + region_of(row_index, lat_total, WIN_LAT)[None, :, :]
    source_row = (row_index + WIN_LAT // 2) % lat_total
    lookup = (source_row[:, :, None] == jnp.arange(lat_total, dtype=jnp.int32)[None, None, :]).astype(jnp.int32)
    usable = lax.optimization_barrier(jnp.sum(lookup * pad_mask[None, None, :], axis=-1)) == 1
    return (region[:, :, :, None] == region[:, :, None, :]) & usable[None, :, None, :]

def earth_bias(bias_table, index_table):
    gathered = jnp.take(bias_table, index_table, axis=3).astype(jnp.float32)
    return jnp.transpose(gathered, (1, 0, 2, 3, 4))

def to_windows(layout):
    levels, lat_rows, lon_columns, channels = layout.shape
    shaped = layout.reshape(levels // WIN_Z, WIN_Z, lat_rows // WIN_LAT, WIN_LAT, lon_columns // WIN_LON, WIN_LON, channels)
    shaped = shaped.transpose(0, 2, 4, 1, 3, 5, 6)
    return shaped.reshape(levels // WIN_Z, lat_rows // WIN_LAT, lon_columns // WIN_LON, WIN_TOK, channels)

def from_windows(window_tiles):
    z_windows, lat_windows, lon_windows, tokens, channels = window_tiles.shape
    shaped = window_tiles.reshape(z_windows, lat_windows, lon_windows, WIN_Z, WIN_LAT, WIN_LON, channels)
    shaped = shaped.transpose(0, 3, 1, 4, 2, 5, 6)
    return shaped.reshape(z_windows * WIN_Z, lat_windows * WIN_LAT, lon_windows * WIN_LON, channels)

def attend(projections, bias_full, allowed):
    pieces = projections.astype(jnp.float32).reshape(projections.shape[:-1] + (3, HEADS, HEAD_DIM))
    queries = pieces[..., 0, :, :]
    key_rows = pieces[..., 1, :, :]
    value_rows = pieces[..., 2, :, :]
    scores = jnp.einsum('abthd,abuhd->abhtu', queries, key_rows) / jnp.sqrt(jnp.float32(HEAD_DIM)) + bias_full
    scores = jnp.where(allowed[:, :, None], scores, -jnp.inf)
    largest = lax.optimization_barrier(jnp.max(scores, axis=-1, keepdims=True))
    powers = jnp.exp(scores - largest)
    weights = (powers / lax.optimization_barrier(jnp.sum(powers, axis=-1, keepdims=True))).astype(jnp.bfloat16)
    attended = jnp.einsum('abhtu,abuhd->abthd', weights.astype(jnp.float32), value_rows).astype(jnp.bfloat16)
    return attended.reshape(attended.shape[:3] + (HEADS * HEAD_DIM,))

def finish(attended, w_proj, proj_bias, norm_gain, norm_shift):
    projected = jnp.dot(attended, w_proj, preferred_element_type=jnp.float32) + proj_bias
    average = lax.optimization_barrier(jnp.mean(projected, axis=-1, keepdims=True))
    centered = projected - average
    spread = lax.optimization_barrier(jnp.mean(centered * centered, axis=-1, keepdims=True))
    return centered * lax.rsqrt(spread + norm_epsilon) * norm_gain + norm_shift

def reference(state_tokens, land_mask, pad_mask, land_embed, w_qkv, w_proj, proj_bias, norm_gain, norm_shift, bias_table, index_table):
    embedded = jnp.where(land_mask[:, :, None] == 1, land_embed[1], land_embed[0])
    hidden = (state_tokens.astype(jnp.float32) + embedded[None]).astype(jnp.bfloat16)
    shifted = jnp.roll(hidden, (-(WIN_Z // 2), -(WIN_LAT // 2), -(WIN_LON // 2)), axis=(0, 1, 2))
    windows = jnp.moveaxis(to_windows(shifted), 2, 0)
    bias_full = earth_bias(bias_table, index_table)
    allowed = window_rules(LEVELS, 0, LAT, LAT, pad_mask)

    def one_column(column_block):
        projections = jnp.dot(column_block, w_qkv, preferred_element_type=jnp.float32).astype(jnp.bfloat16)
        return finish(attend(projections, bias_full, allowed), w_proj, proj_bias, norm_gain, norm_shift)
    normed = lax.map(one_column, windows)
    layout = from_windows(jnp.moveaxis(normed, 0, 2))
    restored = jnp.roll(layout, (WIN_Z // 2, WIN_LAT // 2, WIN_LON // 2), axis=(0, 1, 2))
    return (hidden.astype(jnp.float32) + restored).astype(jnp.bfloat16)
```

```python
import functools

import jax
import jax.numpy as jnp
import numpy as np
from jax import lax
from jax.experimental import pallas as pl
from jax.experimental.pallas import tpu as pltpu
from jax.sharding import PartitionSpec as P

HEADS = 12
HEAD_DIM = 32
WIN_Z = 2
WIN_LAT = 6
WIN_LON = 12
WIN_TOK = 144
HALF_LAT = WIN_LAT // 2
HALF_LON = WIN_LON // 2
GROUP = WIN_Z * HALF_LAT * HALF_LON
PAIR = WIN_Z * GROUP
SLOT = 48
EDGE_ROWS = 80
LOW = 256
SHUT = -1e30
WIDTH = HEADS * HEAD_DIM
MESH = pl.DeviceIdType.MESH

norm_epsilon = 1e-05


def group_tokens(a, b):
    dz, di, dj = np.meshgrid(
        np.arange(WIN_Z), np.arange(HALF_LAT), np.arange(HALF_LON), indexing="ij"
    )
    return ((dz * WIN_LAT + a * HALF_LAT + di) * WIN_LON + b * HALF_LON + dj).reshape(-1)


def window_orders():
    groups = [group_tokens(a, b) for a in range(2) for b in range(2)]
    queries = np.concatenate(groups)
    keys = np.concatenate([g[:32] for g in groups] + [g[32:] for g in groups])
    return queries, keys


def dot(x, y):
    return jnp.dot(x, y, preferred_element_type=jnp.float32)


def iota(shape, axis):
    return lax.broadcasted_iota(jnp.int32, shape, axis)


def index_planes(index_ref, to_q_ref, to_k_ref, to_q_rest_ref, to_k_rest_ref, low_ref, high_ref):
    index = index_ref[...]
    rest_lane = iota((160, LOW), 1) // 16
    rest_row = iota((160, LOW), 0) % 16
    gather = jnp.where(iota((16, 160), 1) // 16 == iota((16, 160), 0), 1.0, 0.0)
    gather = gather.astype(jnp.bfloat16)
    for values, ref in ((index % LOW, low_ref), (index // LOW, high_ref)):
        values = values.astype(jnp.float32).astype(jnp.bfloat16)
        main = dot(dot(to_q_ref[...], values).astype(jnp.bfloat16), to_k_ref[...])
        ref[0:WIN_TOK, :] = main.astype(jnp.int32)
        rest = dot(dot(to_q_rest_ref[...], values).astype(jnp.bfloat16), to_k_rest_ref[...])
        rest = jnp.where(rest_lane == rest_row, rest, 0.0).astype(jnp.bfloat16)
        rest = dot(gather, rest).astype(jnp.int32)
        ref[WIN_TOK : WIN_TOK + 16, :] = rest[:, 0:128]
        ref[WIN_TOK + 16 : WIN_TOK + 32, :] = rest[:, 128:256]


def stack_tables(before_ref, own_ref, table_ref):
    positions = own_ref.shape[-1]
    for k in range(table_ref.shape[1] // 48):
        end = min(positions, (k + 1) * LOW)
        sides = []
        for window in range(3):
            parts = []
            for zw in range(WIN_Z):
                ref = before_ref if window == 0 else own_ref.at[window - 1]
                part = ref[zw, :, k * LOW : end].astype(jnp.float32)
                if end < (k + 1) * LOW:
                    fill = jnp.zeros((part.shape[0], (k + 1) * LOW - end), jnp.float32)
                    part = jnp.concatenate([part, fill], axis=1)
                parts.append(part)
            sides.append([parts[0][:8], parts[1][:8], parts[0][8:], parts[1][8:]])
        for a, edge in ((0, 2), (1, 0)):
            block = jnp.concatenate(sides[edge] + sides[1], axis=0)
            table_ref[a, k * 48 : (k + 1) * 48, :] = block.astype(jnp.bfloat16)


def look_up_bias(a, lat, pad_ref, geometry_ref, low_ref, high_ref, table_ref, bias_ref):
    highs = table_ref.shape[1] // 48
    lat_total = pad_ref.shape[0]
    windows = lat_total // WIN_LAT
    half_row = iota((8, LOW), 0) < 4
    low_iota = iota((LOW, LOW), 0)

    def look_up(tile, low, high):
        hot = jnp.where(low_iota == low, 1.0, 0.0).astype(jnp.bfloat16)
        found = dot(table_ref[a], hot)
        high = jnp.broadcast_to(high, (8, LOW))
        total = [found[8 * j : 8 * j + 8] for j in range(6)]
        for k in range(1, highs):
            here = high == k
            for j in range(6):
                row = k * 48 + 8 * j
                total[j] = jnp.where(here, found[row : row + 8], total[j])
        geometry = geometry_ref[tile]
        key_row, same_half, same_level = geometry[0:1], geometry[1:2], geometry[2:3]
        pieces = []
        for s in range(2):
            window = 2 * lat
            if s == 0:
                window = lax.rem(2 * lat - 1 + windows if a == 1 else 2 * lat + 1, windows)
            usable = jnp.zeros((1, LOW), jnp.int32)
            for n in range(WIN_LAT):
                source = lax.rem(window * WIN_LAT + n + HALF_LAT, lat_total)
                usable = jnp.where(key_row == n, pad_ref[source], usable)
            inner = (window != windows - 1).astype(jnp.int32)
            usable = jnp.where(usable == 1, jnp.maximum(same_half, inner), 0)
            first = jnp.broadcast_to(usable, (8, LOW))
            second = jnp.broadcast_to(usable * same_level, (8, LOW))
            for kind, allowed in enumerate((first, second, jnp.where(half_row, first, second))):
                pieces.append(jnp.where(allowed == 1, total[s * 3 + kind], SHUT))
        return pieces

    def pair(p, carry):
        tile = a * 36 + p

        def two(ref):
            return jnp.concatenate(
                [ref[pl.ds(2 * tile, 1), :], ref[pl.ds(2 * tile + 1, 1), :]], axis=1
            )

        pieces = look_up(tile, two(low_ref), two(high_ref))
        for s in range(2):
            for kind in range(3):
                part = pieces[s * 3 + kind]
                bias_ref[a, s, kind, 2 * p, :, 0:128] = part[:, 0:128]
                bias_ref[a, s, kind, 2 * p + 1, :, 0:128] = part[:, 128:256]
        return carry

    lax.fori_loop(0, 36, pair, 0, unroll=2)
    for tile in range(5):
        row = WIN_TOK + a * 5 + tile

        def wide(ref, row=row):
            return jnp.concatenate([ref[row : row + 1, :], ref[row + 16 : row + 17, :]], axis=1)

        pieces = look_up(72 + a * 5 + tile, wide(low_ref), wide(high_ref))
        for j in range(16):
            q = tile * 16 + j
            if q < 72:
                for s in range(2):
                    for kind in range(3):
                        part = pieces[s * 3 + kind]
                        bias_ref[a, s, kind, q, :, 128:144] = part[:, 16 * j : 16 * j + 16]


def layer_kernel(
    state_hbm,
    w_qkv_hbm,
    w_proj_hbm,
    table_own_ref,
    index_ref,
    pad_ref,
    land_mask_ref,
    land_embed_ref,
    offset_ref,
    gain_ref,
    shift_ref,
    pick_ref,
    restore_ref,
    to_q_ref,
    to_k_ref,
    to_q_rest_ref,
    to_k_rest_ref,
    geometry_ref,
    out_ref,
    state_ref,
    w_qkv_ref,
    w_proj_ref,
    before_ref,
    hidden_ref,
    tokens_ref,
    from_lon_ref,
    from_lat_ref,
    queries_ref,
    keys_ref,
    tails_ref,
    low_ref,
    high_ref,
    table_ref,
    bias_ref,
    attended_ref,
    local_sem,
    send_sem,
    recv_sem,
    table_sem,
    lat_send_sem,
    lat_recv_sem,
):
    lat = lax.axis_index("lat")
    lon = lax.axis_index("lon")
    lon_count = lax.axis_size("lon")
    other = 1 - lat
    left = lax.rem(lon + lon_count - 1, lon_count)
    right = lax.rem(lon + 1, lon_count)
    loads = [
        pltpu.make_async_copy(source, target, local_sem.at[n])
        for n, (source, target) in enumerate(
            ((state_hbm, state_ref), (w_qkv_hbm, w_qkv_ref), (w_proj_hbm, w_proj_ref))
        )
    ]
    for load in loads:
        load.start()
    barrier = pltpu.get_barrier_semaphore()
    for device in ({"lon": left}, {"lon": right}, {"lat": other}):
        pl.semaphore_signal(barrier, inc=1, device_id=device, device_id_type=MESH)

    levels, lat_rows, lon_columns, features = state_ref.shape
    hidden_ref[:, :, 8:16, :] = jnp.zeros((levels, lat_rows, 8, features), jnp.bfloat16)
    loads[0].wait()

    eye = iota((lon_columns, lon_columns), 0) == iota((lon_columns, lon_columns), 1)

    def embed(i, carry):
        row = jnp.broadcast_to(land_mask_ref[pl.ds(i, 1), :], (lon_columns, lon_columns))
        row = jnp.where(eye, row.astype(jnp.float32), 0.0)
        land = jnp.sum(row, axis=1, keepdims=True) > 0.5
        embedded = jnp.where(land, land_embed_ref[1:2, :], land_embed_ref[0:1, :])
        for z in range(levels):
            hidden = state_ref[z, i].astype(jnp.float32) + embedded
            hidden_ref[z, i, 0:lon_columns, :] = hidden.astype(jnp.bfloat16)
        return carry

    lax.fori_loop(0, lat_rows, embed, 0)

    edge = 3 * other
    wrap = 3 * lat
    quarters = (edge, wrap, 1, 2)
    halves = (lat, other, 0, 1)

    def group(quarter):
        rows = [
            hidden_ref[z, pl.ds(quarter * HALF_LAT, HALF_LAT)].reshape(SLOT, features)
            for z in range(levels)
        ]
        return dot(pick_ref[...], jnp.concatenate(rows, axis=0))

    def group_pair(n):
        first, second = group(quarters[2 * n]), group(quarters[2 * n + 1])
        for side in range(2):
            part = slice(side * PAIR, (side + 1) * PAIR)
            both = jnp.concatenate([first[part], second[part]], axis=0)
            tokens_ref[side, 2 * n * PAIR : 2 * (n + 1) * PAIR] = both.astype(jnp.bfloat16)

    pieces = ((0, 80), (144, 80), (224, 64), (80, 64))

    def lon_copy(side, n):
        start, size = pieces[n]
        return pltpu.make_async_remote_copy(
            src_ref=tokens_ref.at[side, pl.ds(start, size)],
            dst_ref=from_lon_ref.at[1 - side, pl.ds(start, size)],
            send_sem=send_sem.at[side, n],
            recv_sem=recv_sem.at[1 - side, n],
            device_id={"lon": right if side == 1 else left},
            device_id_type=MESH,
        )

    def lat_copy(column):
        source = tokens_ref.at[column - 1] if column in (1, 2) else from_lon_ref.at[column // 3]
        return pltpu.make_async_remote_copy(
            src_ref=source.at[pl.ds(0, EDGE_ROWS)],
            dst_ref=from_lat_ref.at[column],
            send_sem=lat_send_sem.at[column],
            recv_sem=lat_recv_sem.at[column],
            device_id={"lat": other},
            device_id_type=MESH,
        )

    table_copy = pltpu.make_async_remote_copy(
        src_ref=table_own_ref.at[1],
        dst_ref=before_ref,
        send_sem=table_sem.at[0],
        recv_sem=table_sem.at[1],
        device_id={"lat": other},
        device_id_type=MESH,
    )

    group_pair(0)
    pl.semaphore_wait(barrier, 3)
    for side in (1, 0):
        lon_copy(side, 0).start()
    table_copy.start()
    group_pair(1)
    for n in range(1, 4):
        for side in (1, 0):
            lon_copy(side, n).start()
    for column in (1, 2):
        lat_copy(column).start()

    def place(values, window, side, a, b):
        row = pl.multiple_of(32 * (2 * a + b), 32)
        for zw in range(2):
            part = values[32 * zw : 32 * zw + 32].astype(jnp.bfloat16)
            keys_ref[window, side, zw, pl.ds(row, 32), :] = part
        tails_ref[window, side, 2 * a + b] = values[64:72]

    def place_pair(values, n, side, b):
        for m in range(2):
            slot = 2 * n + m
            place(values[m * PAIR : (m + 1) * PAIR], min(slot, 2), side, halves[slot], b)

    lower = iota((8, 2 * WIDTH), 0) < 4

    def place_tails(window, side):
        t = [tails_ref[window, side, n] for n in range(4)]
        for zw in range(2):
            rows = []
            for n in (0, 2):
                x, y = t[n], t[n + 1]
                if zw == 0:
                    y = pltpu.roll(y, 4, 0)
                else:
                    x = pltpu.roll(x, 4, 0)
                rows.append(jnp.where(lower, x, y))
            keys_ref[window, side, zw, 128:144, :] = jnp.concatenate(rows, axis=0).astype(
                jnp.bfloat16
            )

    index_planes(
        index_ref, to_q_ref, to_k_ref, to_q_rest_ref, to_k_rest_ref, low_ref, high_ref
    )
    for side in range(2):
        empty = pl.multiple_of(64 * lat, 64)
        for zw in range(2):
            keys_ref[1, side, zw, pl.ds(empty, 64), :] = jnp.zeros((64, 2 * WIDTH), jnp.bfloat16)
        for b in range(2):
            tails_ref[1, side, 2 * lat + b] = jnp.zeros((8, 2 * WIDTH), jnp.float32)

    loads[1].wait()
    for side in range(2):
        for n in range(2):
            tokens = tokens_ref[side, 2 * n * PAIR : 2 * (n + 1) * PAIR]
            qkv = dot(tokens, w_qkv_ref[...])
            for m in range(2):
                part = qkv[m * PAIR : (m + 1) * PAIR, 0:WIDTH]
                for zw in range(2):
                    main = part[32 * zw : 32 * zw + 32].astype(jnp.bfloat16)
                    tail = part[64 + 4 * zw : 68 + 4 * zw].astype(jnp.bfloat16)
                    queries_ref[side, 2 * n + m, zw, 0:32] = main
                    queries_ref[side, 2 * n + m, zw, 32:36] = tail
            place_pair(qkv[:, WIDTH:], n, side, 1 - side)

    table_copy.wait()
    stack_tables(before_ref, table_own_ref, table_ref)
    look_up_bias(0, lat, pad_ref, geometry_ref, low_ref, high_ref, table_ref, bias_ref)
    for side in range(2):
        lon_copy(1 - side, 0).wait_recv()
    for column in (0, 3):
        lat_copy(column).start()
    look_up_bias(1, lat, pad_ref, geometry_ref, low_ref, high_ref, table_ref, bias_ref)

    def project(tokens):
        return dot(tokens, w_qkv_ref[:, WIDTH : 3 * WIDTH])

    for column in range(4):
        lat_copy(column).wait_recv()
        values = project(from_lat_ref[column])
        place(values, 0, column // 2, other, column % 2)
    for n in (1, 2, 3):
        for side in range(2):
            lon_copy(1 - side, n).wait_recv()
    for n in (0, 1):
        for side in range(2):
            values = project(from_lon_ref[side, 2 * n * PAIR : 2 * (n + 1) * PAIR])
            place_pair(values, n, side, side)
    for window in range(3):
        for side in range(2):
            place_tails(window, side)

    head_mask = jnp.where(iota((8, 256), 1) // HEAD_DIM == iota((8, 256), 0), 1.0, 0.0)
    gather_rows = jnp.where(
        iota((SLOT, 8 * GROUP), 1) // 8 == iota((SLOT, 8 * GROUP), 0), 1.0, 0.0
    ).astype(jnp.bfloat16)

    def attend(step, carry):
        slot, side = step // 2, lax.rem(step, 2)
        window = jnp.minimum(slot, 2)
        a = jnp.where(slot == 0, lat, jnp.where(slot == 1, other, slot - 2))
        edge_kind = jnp.where(slot < 2, 0, 1)
        first = pl.multiple_of((1 - side) * GROUP, GROUP)
        results = []
        for kind in range(3):
            if kind < 2:
                q = queries_ref[side, slot, kind, :, 0:256]
                key = keys_ref[window, side, kind, :, 0:256]
                value = keys_ref[window, side, kind, :, WIDTH : WIDTH + 256]
            else:
                q, key, value = (
                    jnp.concatenate([ref[0, :, n : n + 128], ref[1, :, n : n + 128]], axis=1)
                    for ref, n in (
                        (queries_ref.at[side, slot], 256),
                        (keys_ref.at[window, side], 256),
                        (keys_ref.at[window, side], 640),
                    )
                )
            q = q.astype(jnp.float32)[0:GROUP]
            spread = (q[:, None, :] * head_mask[None]).reshape(8 * GROUP, 256)
            scores = lax.dot_general(
                spread.astype(jnp.bfloat16),
                key,
                (((1,), (1,)), ((), ())),
                preferred_element_type=jnp.float32,
            )
            bias = bias_ref[a, edge_kind, kind, pl.ds(first, GROUP)]
            bias = bias.reshape(8 * GROUP, 256)[:, 0:WIN_TOK]
            scores = scores * (HEAD_DIM**-0.5) + bias
            powers = jnp.exp(scores - jnp.max(scores, axis=-1, keepdims=True))
            weights = (powers / jnp.sum(powers, axis=-1, keepdims=True)).astype(jnp.bfloat16)
            mixed = dot(weights, value)
            mixed = (mixed.reshape(GROUP, 8, 256) * head_mask[None]).reshape(8 * GROUP, 256)
            results.append(dot(gather_rows, mixed.astype(jnp.bfloat16)).astype(jnp.bfloat16))
        for zw in range(2):
            row = pl.multiple_of((side * 2 + zw) * SLOT, SLOT)
            attended_ref[slot, pl.ds(row, SLOT), 0:256] = results[zw]
            attended_ref[slot, pl.ds(row, SLOT), 256:384] = results[2][
                :, zw * 128 : zw * 128 + 128
            ]
        return carry

    lax.fori_loop(0, 8, attend, 0)
    loads[2].wait()

    def finish(slot, carry):
        quarter = jnp.where(slot == 0, edge, jnp.where(slot == 1, wrap, slot - 1))
        natural = dot(restore_ref[...], attended_ref[slot]).astype(jnp.bfloat16)
        projected = dot(natural, w_proj_ref[...]) + offset_ref[...]
        centered = projected - jnp.mean(projected, axis=-1, keepdims=True)
        spread = jnp.mean(centered * centered, axis=-1, keepdims=True)
        normed = centered * lax.rsqrt(spread + norm_epsilon) * gain_ref[...] + shift_ref[...]
        normed = normed.reshape(levels, HALF_LAT, 16, features)
        rows = pl.ds(quarter * HALF_LAT, HALF_LAT)
        hidden = hidden_ref[:, rows].astype(jnp.float32)
        result = (hidden + normed).astype(jnp.bfloat16)
        out_ref[:, rows] = result[:, :, 0:lon_columns, :]
        return carry

    lax.fori_loop(0, 4, finish, 0)

    table_copy_done = table_copy
    for side in range(2):
        for n in range(4):
            lon_copy(side, n).wait_send()
    for column in range(4):
        lat_copy(column).wait_send()


def as_tiles(rows):
    main = rows[:, :128].reshape(72, 256)
    rest = np.pad(rows[:, 128:].reshape(2, 72, 16), ((0, 0), (0, 8), (0, 0))).reshape(10, 256)
    return np.concatenate([main, rest], axis=0)


def bias_constants():
    queries, keys = window_orders()
    eye = np.eye(WIN_TOK, dtype=np.float32)
    to_q = eye[queries]
    to_q_rest = np.pad(to_q.reshape(2, 72, WIN_TOK), ((0, 0), (0, 8), (0, 0)))
    to_q_rest = to_q_rest.reshape(160, WIN_TOK)
    to_k = eye[keys[:128]].T
    to_k_rest = eye[np.tile(keys[128:], 16)].T
    q_level, q_half = queries // 72, queries // 12 % 6 // 3
    k_level, k_row = keys // 72, keys // 12 % 6
    planes = [
        np.broadcast_to(k_row[None, :], (WIN_TOK, WIN_TOK)),
        q_half[:, None] == (k_row // 3)[None, :],
        q_level[:, None] == k_level[None, :],
    ]
    geometry = np.stack([as_tiles(p.astype(np.int32)) for p in planes], axis=1)
    matrices = [jnp.asarray(m, jnp.bfloat16) for m in (to_q, to_k, to_q_rest, to_k_rest)]
    return matrices + [jnp.asarray(geometry)]


def group_constants(levels, columns):
    pick = np.zeros((2 * PAIR, levels * SLOT), np.float32)
    restore = np.zeros((levels * SLOT, 2 * WIN_Z * SLOT), np.float32)
    for side in range(2):
        for zw in range(WIN_Z):
            for t in range(GROUP):
                dz, rest = divmod(t, HALF_LAT * HALF_LON)
                di, dj = divmod(rest, HALF_LON)
                z = (WIN_Z * zw + dz + WIN_Z // 2) % levels
                natural = (z * HALF_LAT + di) * 16 + side * HALF_LON + dj
                place = 32 * zw + t if t < 32 else 64 + 4 * zw + t - 32
                pick[side * PAIR + place, natural] = 1.0
                restore[natural, (side * WIN_Z + zw) * SLOT + t] = 1.0
    return jnp.asarray(pick, jnp.bfloat16), jnp.asarray(restore, jnp.bfloat16)


def on_device(
    state_tokens,
    land_mask,
    pad_mask,
    land_embed,
    w_qkv,
    w_proj,
    proj_bias,
    norm_gain,
    norm_shift,
    bias_table,
    index_table,
):
    levels, lat_rows, lon_columns, features = state_tokens.shape
    assert (levels, lat_rows, lon_columns) == (2 * WIN_Z, 2 * WIN_LAT, WIN_LON)
    assert lax.axis_size("lat") == 2 and lax.axis_size("lon") > 2
    highs = -(-bias_table.shape[-1] // LOW)
    vectors = [v.reshape(1, features) for v in (proj_bias, norm_gain, norm_shift)]
    constants = [*group_constants(levels, lon_columns), *bias_constants()]
    hbm = pl.BlockSpec(memory_space=pl.ANY)
    vmem = pl.BlockSpec(memory_space=pltpu.VMEM)
    smem = pl.BlockSpec(memory_space=pltpu.SMEM)
    bf16, f32, i32 = jnp.bfloat16, jnp.float32, jnp.int32
    dma = pltpu.SemaphoreType.DMA
    return pl.pallas_call(
        layer_kernel,
        out_shape=jax.ShapeDtypeStruct(state_tokens.shape, bf16),
        in_specs=[hbm] * 3 + [vmem] * 2 + [smem] + [vmem] * 12,
        out_specs=vmem,
        scratch_shapes=[
            pltpu.VMEM(state_tokens.shape, bf16),
            pltpu.VMEM(w_qkv.shape, bf16),
            pltpu.VMEM(w_proj.shape, bf16),
            pltpu.VMEM(bias_table.shape[1:], bf16),
            pltpu.VMEM((levels, lat_rows, 16, features), bf16),
            pltpu.VMEM((2, 4 * PAIR, features), bf16),
            pltpu.VMEM((2, 4 * PAIR, features), bf16),
            pltpu.VMEM((4, EDGE_ROWS, features), bf16),
            pltpu.VMEM((2, 4, WIN_Z, SLOT, WIDTH), bf16),
            pltpu.VMEM((3, 2, WIN_Z, WIN_TOK, 2 * WIDTH), bf16),
            pltpu.VMEM((3, 2, 4, 8, 2 * WIDTH), f32),
            pltpu.VMEM((WIN_TOK + 32, 128), i32),
            pltpu.VMEM((WIN_TOK + 32, 128), i32),
            pltpu.VMEM((2, highs * 48, LOW), bf16),
            pltpu.VMEM((2, 2, 3, 2 * GROUP, 8, 256), f32),
            pltpu.VMEM((4, 4 * SLOT, WIDTH), bf16),
            dma((3,)),
            dma((2, 4)),
            dma((2, 4)),
            dma((2,)),
            dma((4,)),
            dma((4,)),
        ],
        compiler_params=pltpu.CompilerParams(
            collective_id=0, has_side_effects=True, vmem_limit_bytes=56 << 20
        ),
        name="layer",
    )(
        state_tokens,
        w_qkv,
        w_proj,
        bias_table,
        index_table,
        pad_mask,
        land_mask,
        land_embed,
        *vectors,
        *constants,
    )


def solution(mesh):
    in_specs = (
        P("member", "lat", "lon", None),
        P("lat", "lon"),
        P(),
        P(),
        P(),
        P(),
        P(),
        P(),
        P(),
        P("lat", None, None, None),
        P(),
    )
    out_specs = P("member", "lat", "lon", None)
    return jax.shard_map(
        on_device, mesh=mesh, in_specs=in_specs, out_specs=out_specs, check_vma=False
    )
```

```python
import functools

import jax
import jax.numpy as jnp
import numpy as np
from jax import lax
from jax.experimental import pallas as pl
from jax.experimental.pallas import tpu as pltpu
from jax.sharding import PartitionSpec as P

HEADS = 12
HEAD_DIM = 32
WIN_Z = 2
WIN_LAT = 6
WIN_LON = 12
WIN_TOK = 144
HALF_LAT = WIN_LAT // 2
HALF_LON = WIN_LON // 2
GROUP = WIN_Z * HALF_LAT * HALF_LON
PAIR = WIN_Z * GROUP
SLOT = 48
BLOCK = 48
EDGE_ROWS = 80
LOW = 256
SHUT = -1e30
LOG2E = 1.4426950408889634
WIDTH = HEADS * HEAD_DIM
MESH = pl.DeviceIdType.MESH

norm_epsilon = 1e-05


def group_tokens(a, b):
    dz, di, dj = np.meshgrid(
        np.arange(WIN_Z), np.arange(HALF_LAT), np.arange(HALF_LON), indexing="ij"
    )
    return ((dz * WIN_LAT + a * HALF_LAT + di) * WIN_LON + b * HALF_LON + dj).reshape(-1)


def window_orders():
    groups = [group_tokens(a, b) for a in range(2) for b in range(2)]
    queries = np.concatenate(groups)
    keys = np.concatenate([g[:32] for g in groups] + [g[32:] for g in groups])
    return queries, keys


def dot(x, y):
    return jnp.dot(x, y, preferred_element_type=jnp.float32)


def iota(shape, axis):
    return lax.broadcasted_iota(jnp.int32, shape, axis)


def index_planes(index_ref, to_q_ref, to_k_ref, to_q_rest_ref, to_k_rest_ref, low_ref, high_ref):
    index = index_ref[...]
    rest_lane = iota((160, LOW), 1) // 16
    rest_row = iota((160, LOW), 0) % 16
    gather = jnp.where(iota((16, 160), 1) // 16 == iota((16, 160), 0), 1.0, 0.0)
    gather = gather.astype(jnp.bfloat16)
    for values, ref in ((index % LOW, low_ref), (index // LOW, high_ref)):
        values = values.astype(jnp.float32).astype(jnp.bfloat16)
        main = dot(dot(to_q_ref[...], values).astype(jnp.bfloat16), to_k_ref[...])
        ref[0:WIN_TOK, :] = main.astype(jnp.int32)
        rest = dot(dot(to_q_rest_ref[...], values).astype(jnp.bfloat16), to_k_rest_ref[...])
        rest = jnp.where(rest_lane == rest_row, rest, 0.0).astype(jnp.bfloat16)
        rest = dot(gather, rest).astype(jnp.int32)
        ref[WIN_TOK : WIN_TOK + 16, :] = rest[:, 0:128]
        ref[WIN_TOK + 16 : WIN_TOK + 32, :] = rest[:, 128:256]


def stack_tables(before_ref, own_ref, rows_ref, table_ref):
    positions = own_ref.shape[-1]
    heads = own_ref.shape[1]
    for window in range(3):
        ref = before_ref if window == 0 else own_ref.at[window - 1]
        for k in range(table_ref.shape[1] // BLOCK):
            end = min(positions, (k + 1) * LOW)
            for h in range(heads):
                part = ref[h, :, k * LOW : end].astype(jnp.float32)
                if end < (k + 1) * LOW:
                    fill = jnp.zeros((WIN_Z, (k + 1) * LOW - end), jnp.float32)
                    part = jnp.concatenate([part, fill], axis=1)
                row = (k * heads + h) * WIN_Z
                rows_ref[window, row : row + WIN_Z, :] = part
    size = heads * WIN_Z
    for k in range(table_ref.shape[1] // BLOCK):
        own = rows_ref[1, k * size : (k + 1) * size]
        for a, edge in ((0, 2), (1, 0)):
            block = jnp.concatenate([rows_ref[edge, k * size : (k + 1) * size], own], axis=0)
            table_ref[a, k * BLOCK : (k + 1) * BLOCK, :] = block.astype(jnp.bfloat16)


def look_up_bias(a, closed, pad_ref, geometry_ref, low_ref, high_ref, table_ref, bias_ref, halfway):
    highs = table_ref.shape[1] // BLOCK
    lat_total = pad_ref.shape[0]
    odd_row = iota((8, LOW), 0) % 2 == 1
    low_iota = iota((LOW, LOW), 0)

    def look_up(tile, low, high):
        hot = jnp.where(low_iota == low, 1.0, 0.0).astype(jnp.bfloat16)
        found = dot(table_ref[a], hot)
        high = jnp.broadcast_to(high, (8, LOW))
        total = [found[8 * j : 8 * j + 8] for j in range(6)]
        for k in range(1, highs):
            here = high == k
            for j in range(6):
                row = k * BLOCK + 8 * j
                total[j] = jnp.where(here, found[row : row + 8], total[j])
        geometry = geometry_ref[tile]
        key_row, same_half, same_level = geometry[0:1], geometry[1:2], geometry[2:3]
        levels = jnp.where(odd_row, jnp.broadcast_to(same_level, (8, LOW)), 1)
        allowed = [levels, levels]
        if closed:
            usable = jnp.zeros((1, LOW), jnp.int32)
            for n in range(WIN_LAT):
                source = (lat_total - HALF_LAT + n) % lat_total
                usable = jnp.where(key_row == n, pad_ref[source], usable)
            usable = jnp.where(usable == 1, same_half, 0)
            allowed[0] = levels * jnp.broadcast_to(usable, (8, LOW))
        return [
            jnp.where(allowed[s] == 1, total[s * 3 + kind] * LOG2E, SHUT)
            for s in range(2)
            for kind in range(3)
        ]

    def pair(p, carry):
        tile = a * 36 + p

        def two(ref):
            return jnp.concatenate(
                [ref[pl.ds(2 * tile, 1), :], ref[pl.ds(2 * tile + 1, 1), :]], axis=1
            )

        pieces = look_up(tile, two(low_ref), two(high_ref))
        for s in range(2):
            for kind in range(3):
                part = pieces[s * 3 + kind]
                bias_ref[a, s, kind, 2 * p, :, 0:128] = part[:, 0:128]
                bias_ref[a, s, kind, 2 * p + 1, :, 0:128] = part[:, 128:256]
        return carry

    lax.fori_loop(0, 20, pair, 0, unroll=4)
    halfway()
    lax.fori_loop(20, 36, pair, 0, unroll=4)
    for tile in range(5):
        row = WIN_TOK + a * 5 + tile

        def wide(ref, row=row):
            return jnp.concatenate([ref[pl.ds(row, 1), :], ref[pl.ds(row + 16, 1), :]], axis=1)

        pieces = look_up(72 + a * 5 + tile, wide(low_ref), wide(high_ref))
        for j in range(16):
            q = tile * 16 + j
            if q < 72:
                for s in range(2):
                    for kind in range(3):
                        part = pieces[s * 3 + kind]
                        bias_ref[a, s, kind, q, :, 128:144] = part[:, 16 * j : 16 * j + 16]


def layer_kernel(*refs):
    inputs, refs = refs[:18], refs[18:]
    out_hbm, refs = refs[0], refs[1:]
    copies, refs = refs[:18], refs[18:]
    (
        before_ref,
        hidden_ref,
        tokens_ref,
        from_lon_ref,
        from_lat_ref,
        queries_ref,
        keys_ref,
        tails_ref,
        low_ref,
        high_ref,
        rows_ref,
        table_ref,
        bias_ref,
        attended_ref,
        result_ref,
        local_sem,
        out_sem,
        send_sem,
        recv_sem,
        table_sem,
        lat_send_sem,
        lat_recv_sem,
    ) = refs
    lat = lax.axis_index("lat")
    lon = lax.axis_index("lon")
    lon_count = lax.axis_size("lon")
    other = 1 - lat
    left = lax.rem(lon + lon_count - 1, lon_count)
    right = lax.rem(lon + 1, lon_count)
    loads = [
        pltpu.make_async_copy(source, target, local_sem.at[n])
        for n, (source, target) in enumerate(zip(inputs, copies))
    ]
    for load in loads:
        load.start()
    (
        state_ref,
        land_mask_ref,
        land_embed_ref,
        pick_ref,
        w_qkv_ref,
        table_own_ref,
        index_ref,
        to_q_ref,
        to_k_ref,
        to_q_rest_ref,
        to_k_rest_ref,
        geometry_ref,
        pad_ref,
        w_proj_ref,
        offset_ref,
        gain_ref,
        shift_ref,
        restore_ref,
    ) = copies
    barrier = pltpu.get_barrier_semaphore()
    for device in ({"lon": left}, {"lon": right}, {"lat": other}):
        pl.semaphore_signal(barrier, inc=1, device_id=device, device_id_type=MESH)

    lat_rows, lon_columns, levels, features = state_ref.shape
    strip = lon_columns * levels
    part_rows = HALF_LAT * strip
    with jax.named_scope("wait_state"):
        for n in (1, 2, 0):
            loads[n].wait()

    def embed(i, carry):
        sea, land = (
            jnp.broadcast_to(land_embed_ref[n : n + 1, :], (levels, features)) for n in range(2)
        )
        rows = []
        for j in range(lon_columns):
            embedded = jnp.where(land_mask_ref[i, j] == 1, land, sea)
            rows.append(state_ref[i, j].astype(jnp.float32) + embedded)
        hidden = jnp.concatenate(rows, axis=0).astype(jnp.bfloat16).astype(jnp.float32)
        hidden_ref[pl.ds(pl.multiple_of(i * strip, strip), strip), :] = hidden
        return carry

    with jax.named_scope("embed"):
        lax.fori_loop(0, lat_rows, embed, 0)

    edge = 3 * other
    wrap = 3 * lat
    quarters = (edge, wrap, 1, 2)
    halves = (lat, other, 0, 1)
    loads[3].wait()

    def natural_rows(quarter):
        return pl.ds(pl.multiple_of(quarter * part_rows, 16), part_rows)

    def group(quarter):
        return dot(pick_ref[...], hidden_ref[natural_rows(quarter)].astype(jnp.bfloat16))

    def group_pair(n):
        first, second = group(quarters[2 * n]), group(quarters[2 * n + 1])
        for side in range(2):
            part = slice(side * PAIR, (side + 1) * PAIR)
            both = jnp.concatenate([first[part], second[part]], axis=0)
            tokens_ref[side, 2 * n * PAIR : 2 * (n + 1) * PAIR] = both.astype(jnp.bfloat16)

    pieces = ((0, 80), (144, 80), (224, 64), (80, 64))

    far = lax.rem(lon, 2)
    near = 1 - far

    def lon_copy(side, n):
        start, size = pieces[n]
        return pltpu.make_async_remote_copy(
            src_ref=tokens_ref.at[side, pl.ds(start, size)],
            dst_ref=from_lon_ref.at[1 - side, pl.ds(start, size)],
            send_sem=send_sem.at[side, n],
            recv_sem=recv_sem.at[1 - side, n],
            device_id={"lon": jnp.where(side == 1, right, left)},
            device_id_type=MESH,
        )

    def lat_copy(column):
        source = tokens_ref.at[column - 1] if column in (1, 2) else from_lon_ref.at[column // 3]
        return pltpu.make_async_remote_copy(
            src_ref=source.at[pl.ds(0, EDGE_ROWS)],
            dst_ref=from_lat_ref.at[column],
            send_sem=lat_send_sem.at[column],
            recv_sem=lat_recv_sem.at[column],
            device_id={"lat": other},
            device_id_type=MESH,
        )

    table_copy = pltpu.make_async_remote_copy(
        src_ref=table_own_ref.at[1],
        dst_ref=before_ref,
        send_sem=table_sem.at[0],
        recv_sem=table_sem.at[1],
        device_id={"lat": other},
        device_id_type=MESH,
    )

    with jax.named_scope("group0"):
        group_pair(0)
    with jax.named_scope("group1"):
        group_pair(1)

    def place(values, window, side, a, b):
        row = pl.multiple_of(32 * (2 * a + b), 32)
        for zw in range(2):
            part = values[32 * zw : 32 * zw + 32].astype(jnp.bfloat16)
            for n in range(6):
                keys_ref[window, side, n, pl.ds(row, 32), 128 * zw : 128 * zw + 128] = part[
                    :, 128 * n : 128 * n + 128
                ]
        tails_ref[window, side, 2 * a + b] = values[64:72]

    lower = iota((8, 2 * WIDTH), 0) < 4

    def place_tails(window, side):
        t = [tails_ref[window, side, n] for n in range(4)]
        for zw in range(2):
            rows = []
            for n in (0, 2):
                x, y = t[n], t[n + 1]
                if zw == 0:
                    y = pltpu.roll(y, 4, 0)
                else:
                    x = pltpu.roll(x, 4, 0)
                rows.append(jnp.where(lower, x, y))
            both = jnp.concatenate(rows, axis=0).astype(jnp.bfloat16)
            for n in range(6):
                keys_ref[window, side, n, 128:144, 128 * zw : 128 * zw + 128] = both[
                    :, 128 * n : 128 * n + 128
                ]

    with jax.named_scope("planes"):
        for n in range(6, 13):
            loads[n].wait()
        index_planes(
            index_ref, to_q_ref, to_k_ref, to_q_rest_ref, to_k_rest_ref, low_ref, high_ref
        )
    for side in range(2):
        empty = pl.multiple_of(64 * lat, 64)
        for n in range(6):
            keys_ref[1, side, n, pl.ds(empty, 64), :] = jnp.zeros((64, 256), jnp.bfloat16)
        for b in range(2):
            tails_ref[1, side, 2 * lat + b] = jnp.zeros((8, 2 * WIDTH), jnp.float32)

    with jax.named_scope("qkv"):
        loads[4].wait()
        for side in range(2):
            for n in range(2):
                tokens = tokens_ref[side, 2 * n * PAIR : 2 * (n + 1) * PAIR]
                qkv = dot(tokens, w_qkv_ref[...])
                for m in range(2):
                    slot = 2 * n + m
                    part = qkv[m * PAIR : (m + 1) * PAIR]
                    for zw in range(2):
                        main = part[32 * zw : 32 * zw + 32, 0:WIDTH].astype(jnp.bfloat16)
                        tail = part[64 + 4 * zw : 68 + 4 * zw, 0:WIDTH].astype(jnp.bfloat16)
                        for g in range(3):
                            lanes = slice(128 * g, 128 * g + 128)
                            out = slice(128 * zw, 128 * zw + 128)
                            queries_ref[side, slot, g, 0:32, out] = main[:, lanes]
                            queries_ref[side, slot, g, 32:36, out] = tail[:, lanes]
                    place(part[:, WIDTH:], min(slot, 2), side, halves[slot], 1 - side)

    loads[5].wait()
    with jax.named_scope("barrier"):
        pl.semaphore_wait(barrier, 3)
    lon_copy(far, 0).start()
    for n in range(4):
        lon_copy(near, n).start()
    table_copy.start()
    for column in (1, 2):
        lat_copy(column).start()

    with jax.named_scope("stack"):
        table_copy.wait()
        stack_tables(before_ref, table_own_ref, rows_ref, table_ref)

    def bias(a, closed, halfway):
        look_up_bias(
            a, closed, pad_ref, geometry_ref, low_ref, high_ref, table_ref, bias_ref, halfway
        )

    def forward():
        for side in range(2):
            lon_copy(1 - side, 0).wait_recv()
        for column in (0, 3):
            lat_copy(column).start()

    def project(tokens):
        return dot(tokens, w_qkv_ref[:, WIDTH : 3 * WIDTH])

    head_mask = jnp.where(
        (iota((8, 256), 1) // 128 == iota((8, 256), 0) % 2)
        & (iota((8, 256), 1) % 128 // HEAD_DIM == iota((8, 256), 0) // 2),
        1.0,
        0.0,
    )
    gather_rows = jnp.where(
        iota((SLOT, 8 * GROUP), 1) // 8 == iota((SLOT, 8 * GROUP), 0), 1.0, 0.0
    ).astype(jnp.bfloat16)

    def attend(slot, side):
        window = min(slot, 2) if isinstance(slot, int) else 2
        a = halves[slot] if isinstance(slot, int) else slot - 2
        edge_kind = 0 if isinstance(slot, int) and slot < 2 else 1
        first = (1 - side) * GROUP
        for g in range(3):
            key = keys_ref[window, side, g]
            value = keys_ref[window, side, 3 + g]
            q = queries_ref[side, slot, g].astype(jnp.float32)[0:GROUP]
            spread = (q[:, None, :] * head_mask[None]).reshape(8 * GROUP, 256)
            scores = lax.dot_general(
                spread.astype(jnp.bfloat16),
                key,
                (((1,), (1,)), ((), ())),
                preferred_element_type=jnp.float32,
            )
            bias = bias_ref[a, edge_kind, g, pl.ds(first, GROUP)]
            bias = bias.reshape(8 * GROUP, 256)[:, 0:WIN_TOK]
            scores = scores * (HEAD_DIM**-0.5 * LOG2E) + bias
            powers = jnp.exp2(scores - jnp.max(scores, axis=-1, keepdims=True))
            inverse = 1.0 / jnp.sum(powers, axis=-1, keepdims=True)
            weights = (powers * inverse).astype(jnp.bfloat16)
            mixed = dot(weights, value)
            mixed = (mixed.reshape(GROUP, 8, 256) * head_mask[None]).reshape(8 * GROUP, 256)
            part = dot(gather_rows, mixed.astype(jnp.bfloat16)).astype(jnp.bfloat16)
            for zw in range(2):
                row = (side * 2 + zw) * SLOT
                attended_ref[slot, pl.ds(row, SLOT), 128 * g : 128 * g + 128] = part[
                    :, 128 * zw : 128 * zw + 128
                ]

    def attend_sides(slot):
        for side in range(2):
            attend(slot, side)

    offset, gain, shift = offset_ref, gain_ref, shift_ref

    def out_copy(slot):
        rows = pl.ds(quarters[slot] * HALF_LAT, HALF_LAT)
        return pltpu.make_async_copy(result_ref.at[rows], out_hbm.at[rows], out_sem.at[slot])

    def finish(slot):
        quarter = quarters[slot]
        natural = dot(restore_ref[...], attended_ref[slot]).astype(jnp.bfloat16)
        projected = dot(natural, w_proj_ref[...]) + offset[...][None, :]
        centered = projected - jnp.mean(projected, axis=-1, keepdims=True)
        spread = jnp.mean(centered * centered, axis=-1, keepdims=True)
        normed = centered * lax.rsqrt(spread + norm_epsilon) * gain[...][None, :]
        normed = normed + shift[...][None, :]
        result = hidden_ref[natural_rows(quarter)] + normed
        for n in range(HALF_LAT * lon_columns):
            i, j = divmod(n, lon_columns)
            part = result[n * levels : (n + 1) * levels]
            result_ref[quarter * HALF_LAT + i, j] = part.astype(jnp.bfloat16)
        out_copy(slot).start()

    with jax.named_scope("bias_edge"):
        bias(lat, False, lambda: None)
    for n in (1, 2):
        lon_copy(far, n).start()
    with jax.named_scope("bias_wrap"):
        bias(other, True, forward)
    for n in range(13, 18):
        loads[n].wait()
    with jax.named_scope("keys_edge"):
        values = project(from_lon_ref[:, 0:EDGE_ROWS].reshape(2 * EDGE_ROWS, features))
        for side in range(2):
            place(values[EDGE_ROWS * side : EDGE_ROWS * (side + 1)], 0, side, lat, side)
        for column in range(4):
            lat_copy(column).wait_recv()
        values = project(from_lat_ref[...].reshape(4 * EDGE_ROWS, features))
        for column in range(4):
            part = values[EDGE_ROWS * column : EDGE_ROWS * (column + 1)]
            place(part, 0, column // 2, other, column % 2)
        for side in range(2):
            place_tails(0, side)
    with jax.named_scope("attend_edge"):
        attend_sides(0)
    lon_copy(far, 3).start()
    with jax.named_scope("finish_edge"):
        finish(0)
    with jax.named_scope("wait_own"):
        for n in (1, 2):
            for side in range(2):
                lon_copy(1 - side, n).wait_recv()
    with jax.named_scope("keys_own"):
        for side in range(2):
            values = project(from_lon_ref[side, 2 * PAIR : 4 * PAIR])
            for m in range(2):
                place(values[m * PAIR : (m + 1) * PAIR], 2, side, m, side)
            place_tails(2, side)
    with jax.named_scope("attend_own"):
        def own(slot, carry):
            attend_sides(slot)
            return carry

        lax.fori_loop(2, 4, own, 0)
    with jax.named_scope("finish_own"):
        finish(2)
        finish(3)
    with jax.named_scope("wait_wrap"):
        for side in range(2):
            lon_copy(1 - side, 3).wait_recv()
    with jax.named_scope("keys_wrap"):
        for side in range(2):
            values = project(from_lon_ref[side, 64 : 2 * PAIR])
            place(values[8:80], 1, side, other, side)
            place_tails(1, side)
    with jax.named_scope("attend_wrap"):
        attend_sides(1)
    with jax.named_scope("finish_wrap"):
        finish(1)
    with jax.named_scope("drain"):
        for slot in range(4):
            out_copy(slot).wait()
        for side in range(2):
            for n in range(4):
                lon_copy(side, n).wait_send()
        for column in range(4):
            lat_copy(column).wait_send()


def as_tiles(rows):
    main = rows[:, :128].reshape(72, 256)
    rest = np.pad(rows[:, 128:].reshape(2, 72, 16), ((0, 0), (0, 8), (0, 0))).reshape(10, 256)
    return np.concatenate([main, rest], axis=0)


def bias_constants():
    queries, keys = window_orders()
    eye = np.eye(WIN_TOK, dtype=np.float32)
    to_q = eye[queries]
    to_q_rest = np.pad(to_q.reshape(2, 72, WIN_TOK), ((0, 0), (0, 8), (0, 0)))
    to_q_rest = to_q_rest.reshape(160, WIN_TOK)
    to_k = eye[keys[:128]].T
    to_k_rest = eye[np.tile(keys[128:], 16)].T
    q_level, q_half = queries // 72, queries // 12 % 6 // 3
    k_level, k_row = keys // 72, keys // 12 % 6
    planes = [
        np.broadcast_to(k_row[None, :], (WIN_TOK, WIN_TOK)),
        q_half[:, None] == (k_row // 3)[None, :],
        q_level[:, None] == k_level[None, :],
    ]
    geometry = np.stack([as_tiles(p.astype(np.int32)) for p in planes], axis=1)
    matrices = [jnp.asarray(m, jnp.bfloat16) for m in (to_q, to_k, to_q_rest, to_k_rest)]
    return matrices + [jnp.asarray(geometry)]


def group_constants(levels, columns):
    rows = HALF_LAT * columns * levels
    pick = np.zeros((2 * PAIR, rows), np.float32)
    restore = np.zeros((rows, 2 * WIN_Z * SLOT), np.float32)
    for side in range(2):
        for zw in range(WIN_Z):
            for t in range(GROUP):
                dz, rest = divmod(t, HALF_LAT * HALF_LON)
                di, dj = divmod(rest, HALF_LON)
                z = (WIN_Z * zw + dz + WIN_Z // 2) % levels
                natural = (di * columns + side * HALF_LON + dj) * levels + z
                place = 32 * zw + t if t < 32 else 64 + 4 * zw + t - 32
                pick[side * PAIR + place, natural] = 1.0
                restore[natural, (side * WIN_Z + zw) * SLOT + t] = 1.0
    return jnp.asarray(pick, jnp.bfloat16), jnp.asarray(restore, jnp.bfloat16)


def on_device(
    state_tokens,
    land_mask,
    pad_mask,
    land_embed,
    w_qkv,
    w_proj,
    proj_bias,
    norm_gain,
    norm_shift,
    bias_table,
    index_table,
):
    levels, lat_rows, lon_columns, features = state_tokens.shape
    assert (levels, lat_rows, lon_columns) == (2 * WIN_Z, 2 * WIN_LAT, WIN_LON)
    assert lax.axis_size("lat") == 2 and lax.axis_size("lon") > 2
    highs = -(-bias_table.shape[-1] // LOW)
    pick, restore = group_constants(levels, lon_columns)
    to_q, to_k, to_q_rest, to_k_rest, geometry = bias_constants()
    state = state_tokens.transpose(1, 2, 0, 3)
    table = bias_table.transpose(0, 2, 1, 3)
    inputs = [
        state,
        land_mask,
        land_embed,
        pick,
        w_qkv,
        table,
        index_table,
        to_q,
        to_k,
        to_q_rest,
        to_k_rest,
        geometry,
        pad_mask,
        w_proj,
        proj_bias,
        norm_gain,
        norm_shift,
        restore,
    ]
    bf16, f32, i32 = jnp.bfloat16, jnp.float32, jnp.int32
    dma = pltpu.SemaphoreType.DMA
    scalars = (1, 12)
    copies = [
        (pltpu.SMEM if n in scalars else pltpu.VMEM)(x.shape, x.dtype)
        for n, x in enumerate(inputs)
    ]
    hbm = pl.BlockSpec(memory_space=pl.ANY)
    tokens = levels * lat_rows * lon_columns
    out = pl.pallas_call(
        layer_kernel,
        out_shape=jax.ShapeDtypeStruct(state.shape, bf16),
        in_specs=[hbm] * len(inputs),
        out_specs=hbm,
        scratch_shapes=copies
        + [
            pltpu.VMEM(table.shape[1:], bf16),
            pltpu.VMEM((tokens, features), f32),
            pltpu.VMEM((2, 4 * PAIR, features), bf16),
            pltpu.VMEM((2, 4 * PAIR, features), bf16),
            pltpu.VMEM((4, EDGE_ROWS, features), bf16),
            pltpu.VMEM((2, 4, 3, SLOT, 256), bf16),
            pltpu.VMEM((3, 2, 6, WIN_TOK, 256), bf16),
            pltpu.VMEM((3, 2, 4, 8, 2 * WIDTH), f32),
            pltpu.VMEM((WIN_TOK + 32, 128), i32),
            pltpu.VMEM((WIN_TOK + 32, 128), i32),
            pltpu.VMEM((3, highs * BLOCK // 2, LOW), f32),
            pltpu.VMEM((2, highs * BLOCK, LOW), bf16),
            pltpu.VMEM((2, 2, 3, 2 * GROUP, 8, 256), f32),
            pltpu.VMEM((4, 4 * SLOT, WIDTH), bf16),
            pltpu.VMEM(state.shape, bf16),
            dma((len(inputs),)),
            dma((4,)),
            dma((2, 4)),
            dma((2, 4)),
            dma((2,)),
            dma((4,)),
            dma((4,)),
        ],
        compiler_params=pltpu.CompilerParams(
            collective_id=0, has_side_effects=True, vmem_limit_bytes=56 << 20
        ),
        name="layer",
    )(*inputs)
    return out.transpose(2, 0, 1, 3)


def solution(mesh):
    in_specs = (
        P("member", "lat", "lon", None),
        P("lat", "lon"),
        P(),
        P(),
        P(),
        P(),
        P(),
        P(),
        P(),
        P("lat", None, None, None),
        P(),
    )
    out_specs = P("member", "lat", "lon", None)
    return jax.shard_map(
        on_device, mesh=mesh, in_specs=in_specs, out_specs=out_specs, check_vma=False
    )
```

```python
import functools

import jax
import jax.numpy as jnp
import numpy as np
from jax import lax
from jax.experimental import pallas as pl
from jax.experimental.pallas import tpu as pltpu
from jax.sharding import PartitionSpec as P

HEADS = 12
HEAD_DIM = 32
WIN_Z = 2
WIN_LAT = 6
WIN_LON = 12
WIN_TOK = 144
HALF_LAT = WIN_LAT // 2
HALF_LON = WIN_LON // 2
GROUP = WIN_Z * HALF_LAT * HALF_LON
PAIR = WIN_Z * GROUP
SLOT = 48
BLOCK = 48
EDGE_ROWS = 80
LOW = 256
SHUT = -1e30
LOG2E = 1.4426950408889634
SCALE = HEAD_DIM**-0.5 * LOG2E
WIDTH = HEADS * HEAD_DIM
MESH = pl.DeviceIdType.MESH

norm_epsilon = 1e-05


def group_tokens(a, b):
    dz, di, dj = np.meshgrid(
        np.arange(WIN_Z), np.arange(HALF_LAT), np.arange(HALF_LON), indexing="ij"
    )
    return ((dz * WIN_LAT + a * HALF_LAT + di) * WIN_LON + b * HALF_LON + dj).reshape(-1)


def window_orders():
    groups = [group_tokens(a, b) for a in range(2) for b in range(2)]
    queries = np.concatenate(groups)
    keys = np.concatenate([g[:32] for g in groups] + [g[32:] for g in groups])
    return queries, keys


def dot(x, y):
    return jnp.dot(x, y, preferred_element_type=jnp.float32)


def iota(shape, axis):
    return lax.broadcasted_iota(jnp.int32, shape, axis)


def index_planes(index_ref, to_q_ref, to_k_ref, to_q_rest_ref, to_k_rest_ref, low_ref, high_ref):
    index = index_ref[...]
    rest_lane = iota((160, LOW), 1) // 16
    rest_row = iota((160, LOW), 0) % 16
    gather = jnp.where(iota((16, 160), 1) // 16 == iota((16, 160), 0), 1.0, 0.0)
    gather = gather.astype(jnp.bfloat16)
    for values, ref in ((index % LOW, low_ref), (index // LOW, high_ref)):
        values = values.astype(jnp.float32).astype(jnp.bfloat16)
        main = dot(dot(to_q_ref[...], values).astype(jnp.bfloat16), to_k_ref[...])
        ref[0:WIN_TOK, :] = main.astype(jnp.int32)
        rest = dot(dot(to_q_rest_ref[...], values).astype(jnp.bfloat16), to_k_rest_ref[...])
        rest = jnp.where(rest_lane == rest_row, rest, 0.0).astype(jnp.bfloat16)
        rest = dot(gather, rest).astype(jnp.int32)
        ref[WIN_TOK : WIN_TOK + 16, :] = rest[:, 0:128]
        ref[WIN_TOK + 16 : WIN_TOK + 32, :] = rest[:, 128:256]


def stack_tables(a, before_ref, own_ref, rows_ref, table_ref):
    positions = own_ref.shape[-1]
    heads = own_ref.shape[1]
    size = heads * WIN_Z
    edge = 2 - 2 * a
    for window in (edge, 1)[: 2 - a]:
        ref = before_ref if window == 0 else own_ref.at[window - 1]
        for k in range(table_ref.shape[1] // BLOCK):
            end = min(positions, (k + 1) * LOW)
            for h in range(heads):
                part = ref[h, :, k * LOW : end].astype(jnp.float32)
                if end < (k + 1) * LOW:
                    fill = jnp.zeros((WIN_Z, (k + 1) * LOW - end), jnp.float32)
                    part = jnp.concatenate([part, fill], axis=1)
                row = (k * heads + h) * WIN_Z
                rows_ref[window, row : row + WIN_Z, :] = part
    for k in range(table_ref.shape[1] // BLOCK):
        both = [rows_ref[window, k * size : (k + 1) * size] for window in (edge, 1)]
        block = jnp.concatenate(both, axis=0)
        table_ref[a, k * BLOCK : (k + 1) * BLOCK, :] = block.astype(jnp.bfloat16)


def look_up_bias(a, closed, pad_ref, geometry_ref, low_ref, high_ref, table_ref, bias_ref, pause, halfway):
    highs = table_ref.shape[1] // BLOCK
    lat_total = pad_ref.shape[0]
    odd_row = iota((8, LOW), 0) % 2 == 1
    low_iota = iota((LOW, LOW), 0)

    def look_up(tile, low, high):
        hot = jnp.where(low_iota == low, 1.0, 0.0).astype(jnp.bfloat16)
        found = dot(table_ref[a], hot)
        high = jnp.broadcast_to(high, (8, LOW))
        total = [found[8 * j : 8 * j + 8] for j in range(6)]
        for k in range(1, highs):
            here = high == k
            for j in range(6):
                row = k * BLOCK + 8 * j
                total[j] = jnp.where(here, found[row : row + 8], total[j])
        geometry = geometry_ref[tile]
        key_row, same_half, same_level = geometry[0:1], geometry[1:2], geometry[2:3]
        levels = jnp.where(odd_row, jnp.broadcast_to(same_level, (8, LOW)), 1)
        allowed = [levels, levels]
        usable = jnp.zeros((1, LOW), jnp.int32)
        for n in range(WIN_LAT):
            source = (lat_total - HALF_LAT + n) % lat_total
            usable = jnp.where(key_row == n, pad_ref[source], usable)
        usable = jnp.where(usable == 1, same_half, 0)
        usable = jnp.maximum(usable, 1 - closed)
        allowed[0] = levels * jnp.broadcast_to(usable, (8, LOW))
        return [
            jnp.where(allowed[s] == 1, total[s * 3 + kind] * LOG2E, SHUT)
            for s in range(2)
            for kind in range(3)
        ]

    def pair(p, carry):
        tile = a * 36 + p

        def two(ref):
            return jnp.concatenate(
                [ref[pl.ds(2 * tile, 1), :], ref[pl.ds(2 * tile + 1, 1), :]], axis=1
            )

        pieces = look_up(tile, two(low_ref), two(high_ref))
        for s in range(2):
            for kind in range(3):
                part = pieces[s * 3 + kind]
                bias_ref[a, s, kind, 2 * p, :, 0:128] = part[:, 0:128]
                bias_ref[a, s, kind, 2 * p + 1, :, 0:128] = part[:, 128:256]
        return carry

    lax.fori_loop(0, pause, pair, 0, unroll=4)
    halfway()
    lax.fori_loop(pause, 36, pair, 0, unroll=4)
    for tile in range(5):
        row = WIN_TOK + a * 5 + tile

        def wide(ref, row=row):
            return jnp.concatenate([ref[pl.ds(row, 1), :], ref[pl.ds(row + 16, 1), :]], axis=1)

        pieces = look_up(72 + a * 5 + tile, wide(low_ref), wide(high_ref))
        for j in range(16):
            q = tile * 16 + j
            if q < 72:
                for s in range(2):
                    for kind in range(3):
                        part = pieces[s * 3 + kind]
                        bias_ref[a, s, kind, q, :, 128:144] = part[:, 16 * j : 16 * j + 16]


def layer_kernel(*refs):
    inputs, refs = refs[:18], refs[18:]
    out_hbm, refs = refs[0], refs[1:]
    copies, refs = refs[:18], refs[18:]
    (
        before_ref,
        hidden_ref,
        tokens_ref,
        from_lon_ref,
        from_lat_ref,
        queries_ref,
        keys_ref,
        tails_ref,
        low_ref,
        high_ref,
        rows_ref,
        table_ref,
        bias_ref,
        attended_ref,
        scores_ref,
        weights_ref,
        result_ref,
        local_sem,
        out_sem,
        send_sem,
        recv_sem,
        table_sem,
        lat_send_sem,
        lat_recv_sem,
    ) = refs
    lat = lax.axis_index("lat")
    lon = lax.axis_index("lon")
    lon_count = lax.axis_size("lon")
    other = 1 - lat
    left = lax.rem(lon + lon_count - 1, lon_count)
    right = lax.rem(lon + 1, lon_count)
    loads = [
        pltpu.make_async_copy(source, target, local_sem.at[n])
        for n, (source, target) in enumerate(zip(inputs, copies))
    ]
    for load in loads:
        load.start()
    (
        state_ref,
        land_mask_ref,
        land_embed_ref,
        pick_ref,
        w_qkv_ref,
        table_own_ref,
        index_ref,
        to_q_ref,
        to_k_ref,
        to_q_rest_ref,
        to_k_rest_ref,
        geometry_ref,
        pad_ref,
        w_proj_ref,
        offset_ref,
        gain_ref,
        shift_ref,
        restore_ref,
    ) = copies
    barrier = pltpu.get_barrier_semaphore()
    for device in ({"lon": left}, {"lon": right}, {"lat": other}):
        pl.semaphore_signal(barrier, inc=1, device_id=device, device_id_type=MESH)

    lat_rows, lon_columns, levels, features = state_ref.shape
    strip = lon_columns * levels
    part_rows = HALF_LAT * strip
    with jax.named_scope("wait_state"):
        for n in (1, 2, 0):
            loads[n].wait()

    def embed(i, carry):
        sea, land = (
            jnp.broadcast_to(land_embed_ref[n : n + 1, :], (levels, features)) for n in range(2)
        )
        rows = []
        for j in range(lon_columns):
            embedded = jnp.where(land_mask_ref[i, j] == 1, land, sea)
            rows.append(state_ref[i, j].astype(jnp.float32) + embedded)
        hidden = jnp.concatenate(rows, axis=0).astype(jnp.bfloat16).astype(jnp.float32)
        hidden_ref[pl.ds(pl.multiple_of(i * strip, strip), strip), :] = hidden
        return carry

    with jax.named_scope("embed"):
        lax.fori_loop(0, lat_rows, embed, 0)

    edge = 3 * other
    wrap = 3 * lat
    quarters = (edge, wrap, 1, 2)
    halves = (lat, other, 0, 1)
    loads[3].wait()

    def natural_rows(quarter):
        return pl.ds(pl.multiple_of(quarter * part_rows, 16), part_rows)

    def group(quarter):
        return dot(pick_ref[...], hidden_ref[natural_rows(quarter)].astype(jnp.bfloat16))

    def group_pair(n):
        first, second = group(quarters[2 * n]), group(quarters[2 * n + 1])
        for side in range(2):
            part = slice(side * PAIR, (side + 1) * PAIR)
            both = jnp.concatenate([first[part], second[part]], axis=0)
            tokens_ref[side, 2 * n * PAIR : 2 * (n + 1) * PAIR] = both.astype(jnp.bfloat16)

    pieces = ((0, 80), (144, 80), (224, 64), (80, 64))

    far = lax.rem(lon, 2)
    near = 1 - far

    def lon_copy(side, n):
        start, size = pieces[n]
        return pltpu.make_async_remote_copy(
            src_ref=tokens_ref.at[side, pl.ds(start, size)],
            dst_ref=from_lon_ref.at[1 - side, pl.ds(start, size)],
            send_sem=send_sem.at[side, n],
            recv_sem=recv_sem.at[1 - side, n],
            device_id={"lon": jnp.where(side == 1, right, left)},
            device_id_type=MESH,
        )

    def lat_copy(column):
        source = tokens_ref.at[column - 1] if column in (1, 2) else from_lon_ref.at[column // 3]
        return pltpu.make_async_remote_copy(
            src_ref=source.at[pl.ds(0, EDGE_ROWS)],
            dst_ref=from_lat_ref.at[column],
            send_sem=lat_send_sem.at[column],
            recv_sem=lat_recv_sem.at[column],
            device_id={"lat": other},
            device_id_type=MESH,
        )

    table_copy = pltpu.make_async_remote_copy(
        src_ref=table_own_ref.at[1],
        dst_ref=before_ref,
        send_sem=table_sem.at[0],
        recv_sem=table_sem.at[1],
        device_id={"lat": other},
        device_id_type=MESH,
    )

    with jax.named_scope("group0"):
        group_pair(0)
    with jax.named_scope("group1"):
        group_pair(1)

    def place(values, window, side, a, b):
        row = pl.multiple_of(32 * (2 * a + b), 32)
        for zw in range(2):
            part = values[32 * zw : 32 * zw + 32].astype(jnp.bfloat16)
            for n in range(6):
                keys_ref[window, side, n, pl.ds(row, 32), 128 * zw : 128 * zw + 128] = part[
                    :, 128 * n : 128 * n + 128
                ]
        tails_ref[window, side, 2 * a + b] = values[64:72]

    lower = iota((8, 2 * WIDTH), 0) < 4

    def place_tails(window, side):
        t = [tails_ref[window, side, n] for n in range(4)]
        for zw in range(2):
            rows = []
            for n in (0, 2):
                x, y = t[n], t[n + 1]
                if zw == 0:
                    y = pltpu.roll(y, 4, 0)
                else:
                    x = pltpu.roll(x, 4, 0)
                rows.append(jnp.where(lower, x, y))
            both = jnp.concatenate(rows, axis=0).astype(jnp.bfloat16)
            for n in range(6):
                keys_ref[window, side, n, 128:144, 128 * zw : 128 * zw + 128] = both[
                    :, 128 * n : 128 * n + 128
                ]

    with jax.named_scope("planes"):
        for n in range(6, 13):
            loads[n].wait()
        index_planes(
            index_ref, to_q_ref, to_k_ref, to_q_rest_ref, to_k_rest_ref, low_ref, high_ref
        )
    loads[5].wait()
    with jax.named_scope("barrier"):
        pl.semaphore_wait(barrier, 3)
    lon_copy(far, 0).start()
    for n in range(4):
        lon_copy(near, n).start()
    table_copy.start()
    for column in (1, 2):
        lat_copy(column).start()

    for n in range(2):
        for g in range(3):
            scores_ref[n, g, :, 128:256] = jnp.full((8 * GROUP, 128), SHUT, jnp.float32)
    for side in range(2):
        empty = pl.multiple_of(64 * lat, 64)
        for n in range(6):
            keys_ref[1, side, n, pl.ds(empty, 64), :] = jnp.zeros((64, 256), jnp.bfloat16)
        for b in range(2):
            tails_ref[1, side, 2 * lat + b] = jnp.zeros((8, 2 * WIDTH), jnp.float32)

    with jax.named_scope("qkv"):
        loads[4].wait()
        for side in range(2):
            for n in range(2):
                tokens = tokens_ref[side, 2 * n * PAIR : 2 * (n + 1) * PAIR]
                qkv = dot(tokens, w_qkv_ref[...])
                for m in range(2):
                    slot = 2 * n + m
                    part = qkv[m * PAIR : (m + 1) * PAIR]
                    queries = part[:, 0:WIDTH].astype(jnp.bfloat16).astype(jnp.float32)
                    for zw in range(2):
                        main = queries[32 * zw : 32 * zw + 32]
                        tail = queries[64 + 4 * zw : 68 + 4 * zw]
                        for g in range(3):
                            lanes = slice(128 * g, 128 * g + 128)
                            out = slice(128 * zw, 128 * zw + 128)
                            queries_ref[side, slot, g, 0:32, out] = main[:, lanes]
                            queries_ref[side, slot, g, 32:36, out] = tail[:, lanes]
                    place(part[:, WIDTH:], min(slot, 2), side, halves[slot], 1 - side)

    with jax.named_scope("stack"):
        stack_tables(0, before_ref, table_own_ref, rows_ref, table_ref)

    def bias(a, closed, pause, halfway):
        look_up_bias(
            a, closed, pad_ref, geometry_ref, low_ref, high_ref, table_ref, bias_ref, pause, halfway
        )

    def send_own():
        for n in (1, 2):
            lon_copy(far, n).start()

    def forward():
        for side in range(2):
            lon_copy(1 - side, 0).wait_recv()
        for column in (0, 3):
            lat_copy(column).start()

    def project(tokens):
        return dot(tokens, w_qkv_ref[:, WIDTH : 3 * WIDTH])

    head_mask = jnp.where(
        (iota((8, 256), 1) // 128 == iota((8, 256), 0) % 2)
        & (iota((8, 256), 1) % 128 // HEAD_DIM == iota((8, 256), 0) // 2),
        1.0,
        0.0,
    )
    gather_rows = jnp.where(
        iota((SLOT, 8 * GROUP), 1) // 8 == iota((SLOT, 8 * GROUP), 0), 1.0, 0.0
    ).astype(jnp.bfloat16)

    def place_of(step):
        kind, side = step // 2, lax.rem(step, 2)
        slot = jnp.where(kind == 0, 0, jnp.where(kind == 3, 1, kind + 1))
        return slot, side

    def score(step, g):
        slot, side = place_of(step)
        half = jnp.where(slot == 0, lat, jnp.where(slot == 1, other, slot - 2))
        edge_kind = jnp.where(slot < 2, 0, 1)
        window = jnp.minimum(slot, 2)
        first = pl.multiple_of((1 - side) * GROUP, GROUP)
        spread = jnp.concatenate(
            [
                jnp.broadcast_to(queries_ref[side, slot, g, t : t + 1], (8, 256)) * head_mask
                for t in range(GROUP)
            ],
            axis=0,
        )
        scores = lax.dot_general(
            spread.astype(jnp.bfloat16),
            keys_ref[window, side, g],
            (((1,), (1,)), ((), ())),
            preferred_element_type=jnp.float32,
        )
        bias = bias_ref[half, edge_kind, g, pl.ds(first, GROUP)].reshape(8 * GROUP, 256)
        scores_ref[lax.rem(step, 2), g, :, 0:WIN_TOK] = scores * SCALE + bias[:, 0:WIN_TOK]

    def weigh(step, g):
        scores = scores_ref[lax.rem(step, 2), g]
        powers = jnp.exp2(scores - jnp.max(scores, axis=-1, keepdims=True))
        inverse = 1.0 / jnp.sum(powers, axis=-1, keepdims=True)
        weights_ref[lax.rem(step, 2), g] = (powers * inverse).astype(jnp.bfloat16)

    def mix(step, g):
        slot, side = place_of(step)
        window = jnp.minimum(slot, 2)
        weights = weights_ref[lax.rem(step, 2), g, :, 0:WIN_TOK]
        mixed = dot(weights, keys_ref[window, side, 3 + g])
        mixed = (mixed.reshape(GROUP, 8, 256) * head_mask[None]).reshape(8 * GROUP, 256)
        part = dot(gather_rows, mixed.astype(jnp.bfloat16)).astype(jnp.bfloat16)
        for zw in range(2):
            row = pl.multiple_of((side * 2 + zw) * SLOT, SLOT)
            attended_ref[slot, pl.ds(row, SLOT), 128 * g : 128 * g + 128] = part[
                :, 128 * zw : 128 * zw + 128
            ]

    def stages(*parts):
        for g in range(3):
            for stage, step in parts:
                stage(step, g)

    def advance(step, carry):
        stages((weigh, step - 1), (score, step), (mix, step - 2))
        return carry

    offset, gain, shift = offset_ref, gain_ref, shift_ref

    def out_copy(slot):
        rows = pl.ds(quarters[slot] * HALF_LAT, HALF_LAT)
        return pltpu.make_async_copy(result_ref.at[rows], out_hbm.at[rows], out_sem.at[slot])

    def finish(slot):
        quarter = quarters[slot]
        natural = dot(restore_ref[...], attended_ref[slot]).astype(jnp.bfloat16)
        projected = dot(natural, w_proj_ref[...]) + offset[...][None, :]
        centered = projected - jnp.mean(projected, axis=-1, keepdims=True)
        spread = jnp.mean(centered * centered, axis=-1, keepdims=True)
        normed = centered * lax.rsqrt(spread + norm_epsilon) * gain[...][None, :]
        normed = normed + shift[...][None, :]
        result = hidden_ref[natural_rows(quarter)] + normed
        for n in range(HALF_LAT * lon_columns):
            i, j = divmod(n, lon_columns)
            part = result[n * levels : (n + 1) * levels]
            result_ref[quarter * HALF_LAT + i, j] = part.astype(jnp.bfloat16)
        out_copy(slot).start()

    with jax.named_scope("bias_edge"):
        bias(0, (other == 0).astype(jnp.int32), 32, send_own)
    with jax.named_scope("stack2"):
        table_copy.wait()
        stack_tables(1, before_ref, table_own_ref, rows_ref, table_ref)
    with jax.named_scope("bias_wrap"):
        bias(1, (other == 1).astype(jnp.int32), 20, forward)
    for n in range(13, 18):
        loads[n].wait()
    with jax.named_scope("keys_edge"):
        values = project(from_lon_ref[:, 0:EDGE_ROWS].reshape(2 * EDGE_ROWS, features))
        for side in range(2):
            place(values[EDGE_ROWS * side : EDGE_ROWS * (side + 1)], 0, side, lat, side)
        for column in range(4):
            lat_copy(column).wait_recv()
        values = project(from_lat_ref[...].reshape(4 * EDGE_ROWS, features))
        for column in range(4):
            part = values[EDGE_ROWS * column : EDGE_ROWS * (column + 1)]
            place(part, 0, column // 2, other, column % 2)
        for side in range(2):
            place_tails(0, side)
    with jax.named_scope("attend_edge"):
        stages((score, 0), (score, 1))
        stages((weigh, 0), (weigh, 1))
        stages((mix, 0), (mix, 1))
    lon_copy(far, 3).start()
    with jax.named_scope("finish_edge"):
        finish(0)
    with jax.named_scope("wait_own"):
        for n in (1, 2):
            for side in range(2):
                lon_copy(1 - side, n).wait_recv()
    with jax.named_scope("keys_own"):
        for side in range(2):
            values = project(from_lon_ref[side, 2 * PAIR : 4 * PAIR])
            for m in range(2):
                place(values[m * PAIR : (m + 1) * PAIR], 2, side, m, side)
            place_tails(2, side)
    with jax.named_scope("attend_own"):
        stages((score, 2))
        stages((weigh, 2), (score, 3))
        lax.fori_loop(4, 6, advance, 0)
        stages((weigh, 5), (mix, 4))
        stages((mix, 5))
    with jax.named_scope("finish_own"):
        finish(2)
        finish(3)
    with jax.named_scope("wait_wrap"):
        for side in range(2):
            lon_copy(1 - side, 3).wait_recv()
    with jax.named_scope("keys_wrap"):
        values = project(from_lon_ref[:, 64 : 2 * PAIR].reshape(2 * EDGE_ROWS, features))
        for side in range(2):
            start = EDGE_ROWS * side + 8
            place(values[start : start + PAIR], 1, side, other, side)
            place_tails(1, side)
    with jax.named_scope("attend_wrap"):
        stages((score, 6), (score, 7))
        stages((weigh, 6), (weigh, 7))
        stages((mix, 6), (mix, 7))
    with jax.named_scope("finish_wrap"):
        finish(1)
    with jax.named_scope("drain"):
        for slot in range(4):
            out_copy(slot).wait()
        for side in range(2):
            for n in range(4):
                lon_copy(side, n).wait_send()
        for column in range(4):
            lat_copy(column).wait_send()


def as_tiles(rows):
    main = rows[:, :128].reshape(72, 256)
    rest = np.pad(rows[:, 128:].reshape(2, 72, 16), ((0, 0), (0, 8), (0, 0))).reshape(10, 256)
    return np.concatenate([main, rest], axis=0)


def bias_constants():
    queries, keys = window_orders()
    eye = np.eye(WIN_TOK, dtype=np.float32)
    to_q = eye[queries]
    to_q_rest = np.pad(to_q.reshape(2, 72, WIN_TOK), ((0, 0), (0, 8), (0, 0)))
    to_q_rest = to_q_rest.reshape(160, WIN_TOK)
    to_k = eye[keys[:128]].T
    to_k_rest = eye[np.tile(keys[128:], 16)].T
    q_level, q_half = queries // 72, queries // 12 % 6 // 3
    k_level, k_row = keys // 72, keys // 12 % 6
    planes = [
        np.broadcast_to(k_row[None, :], (WIN_TOK, WIN_TOK)),
        q_half[:, None] == (k_row // 3)[None, :],
        q_level[:, None] == k_level[None, :],
    ]
    geometry = np.stack([as_tiles(p.astype(np.int32)) for p in planes], axis=1)
    matrices = [jnp.asarray(m, jnp.bfloat16) for m in (to_q, to_k, to_q_rest, to_k_rest)]
    return matrices + [jnp.asarray(geometry)]


def group_constants(levels, columns):
    rows = HALF_LAT * columns * levels
    pick = np.zeros((2 * PAIR, rows), np.float32)
    restore = np.zeros((rows, 2 * WIN_Z * SLOT), np.float32)
    for side in range(2):
        for zw in range(WIN_Z):
            for t in range(GROUP):
                dz, rest = divmod(t, HALF_LAT * HALF_LON)
                di, dj = divmod(rest, HALF_LON)
                z = (WIN_Z * zw + dz + WIN_Z // 2) % levels
                natural = (di * columns + side * HALF_LON + dj) * levels + z
                place = 32 * zw + t if t < 32 else 64 + 4 * zw + t - 32
                pick[side * PAIR + place, natural] = 1.0
                restore[natural, (side * WIN_Z + zw) * SLOT + t] = 1.0
    return jnp.asarray(pick, jnp.bfloat16), jnp.asarray(restore, jnp.bfloat16)


def on_device(
    state_tokens,
    land_mask,
    pad_mask,
    land_embed,
    w_qkv,
    w_proj,
    proj_bias,
    norm_gain,
    norm_shift,
    bias_table,
    index_table,
):
    levels, lat_rows, lon_columns, features = state_tokens.shape
    assert (levels, lat_rows, lon_columns) == (2 * WIN_Z, 2 * WIN_LAT, WIN_LON)
    assert lax.axis_size("lat") == 2 and lax.axis_size("lon") > 2
    highs = -(-bias_table.shape[-1] // LOW)
    pick, restore = group_constants(levels, lon_columns)
    to_q, to_k, to_q_rest, to_k_rest, geometry = bias_constants()
    state = state_tokens.transpose(1, 2, 0, 3)
    table = bias_table.transpose(0, 2, 1, 3)
    inputs = [
        state,
        land_mask,
        land_embed,
        pick,
        w_qkv,
        table,
        index_table,
        to_q,
        to_k,
        to_q_rest,
        to_k_rest,
        geometry,
        pad_mask,
        w_proj,
        proj_bias,
        norm_gain,
        norm_shift,
        restore,
    ]
    bf16, f32, i32 = jnp.bfloat16, jnp.float32, jnp.int32
    dma = pltpu.SemaphoreType.DMA
    scalars = (1, 12)
    copies = [
        (pltpu.SMEM if n in scalars else pltpu.VMEM)(x.shape, x.dtype)
        for n, x in enumerate(inputs)
    ]
    tokens = levels * lat_rows * lon_columns
    out = pl.pallas_call(
        layer_kernel,
        out_shape=pltpu.VMEM(state.shape, bf16),
        in_specs=[pl.BlockSpec(memory_space=pltpu.HBM)] * len(inputs),
        out_specs=pl.BlockSpec(memory_space=pl.ANY),
        scratch_shapes=copies
        + [
            pltpu.VMEM(table.shape[1:], bf16),
            pltpu.VMEM((tokens, features), f32),
            pltpu.VMEM((2, 4 * PAIR, features), bf16),
            pltpu.VMEM((2, 4 * PAIR, features), bf16),
            pltpu.VMEM((4, EDGE_ROWS, features), bf16),
            pltpu.VMEM((2, 4, 3, 40, 256), f32),
            pltpu.VMEM((3, 2, 6, WIN_TOK, 256), bf16),
            pltpu.VMEM((3, 2, 4, 8, 2 * WIDTH), f32),
            pltpu.VMEM((WIN_TOK + 32, 128), i32),
            pltpu.VMEM((WIN_TOK + 32, 128), i32),
            pltpu.VMEM((3, highs * BLOCK // 2, LOW), f32),
            pltpu.VMEM((2, highs * BLOCK, LOW), bf16),
            pltpu.VMEM((2, 2, 3, 2 * GROUP, 8, 256), f32),
            pltpu.VMEM((4, 4 * SLOT, WIDTH), bf16),
            pltpu.VMEM((2, 3, 8 * GROUP, 256), f32),
            pltpu.VMEM((2, 3, 8 * GROUP, 256), bf16),
            pltpu.VMEM(state.shape, bf16),
            dma((len(inputs),)),
            dma((4,)),
            dma((2, 4)),
            dma((2, 4)),
            dma((2,)),
            dma((4,)),
            dma((4,)),
        ],
        compiler_params=pltpu.CompilerParams(
            collective_id=0, has_side_effects=True, vmem_limit_bytes=56 << 20
        ),
        name="layer",
    )(*inputs)
    return out.transpose(2, 0, 1, 3)


def solution(mesh):
    in_specs = (
        P("member", "lat", "lon", None),
        P("lat", "lon"),
        P(),
        P(),
        P(),
        P(),
        P(),
        P(),
        P(),
        P("lat", None, None, None),
        P(),
    )
    out_specs = P("member", "lat", "lon", None)
    return jax.shard_map(
        on_device, mesh=mesh, in_specs=in_specs, out_specs=out_specs, check_vma=False
    )
```

```python
import functools

import jax
import jax.numpy as jnp
import numpy as np
from jax import lax
from jax.experimental import pallas as pl
from jax.experimental.pallas import tpu as pltpu
from jax.sharding import PartitionSpec as P

HEADS = 12
HEAD_DIM = 32
WIN_Z = 2
WIN_LAT = 6
WIN_LON = 12
WIN_TOK = 144
HALF_LAT = WIN_LAT // 2
HALF_LON = WIN_LON // 2
GROUP = WIN_Z * HALF_LAT * HALF_LON
PAIR = WIN_Z * GROUP
SLOT = 48
BLOCK = 48
EDGE_ROWS = 80
LOW = 256
SHUT = -1e30
LOG2E = 1.4426950408889634
SCALE = HEAD_DIM**-0.5 * LOG2E
WIDTH = HEADS * HEAD_DIM
MESH = pl.DeviceIdType.MESH

norm_epsilon = 1e-05


def group_tokens(a, b):
    dz, di, dj = np.meshgrid(
        np.arange(WIN_Z), np.arange(HALF_LAT), np.arange(HALF_LON), indexing="ij"
    )
    return ((dz * WIN_LAT + a * HALF_LAT + di) * WIN_LON + b * HALF_LON + dj).reshape(-1)


def window_orders():
    groups = [group_tokens(a, b) for a in range(2) for b in range(2)]
    queries = np.concatenate(groups)
    keys = np.concatenate([g[:32] for g in groups] + [g[32:] for g in groups])
    return queries, keys


def dot(x, y):
    return jnp.dot(x, y, preferred_element_type=jnp.float32)


def iota(shape, axis):
    return lax.broadcasted_iota(jnp.int32, shape, axis)


def index_planes(index_ref, to_q_ref, to_k_ref, to_q_rest_ref, to_k_rest_ref, low_ref, high_ref):
    index = index_ref[...]
    rest_lane = iota((160, LOW), 1) // 16
    rest_row = iota((160, LOW), 0) % 16
    gather = jnp.where(iota((16, 160), 1) // 16 == iota((16, 160), 0), 1.0, 0.0)
    gather = gather.astype(jnp.bfloat16)
    for values, ref in ((index % LOW, low_ref), (index // LOW, high_ref)):
        values = values.astype(jnp.float32).astype(jnp.bfloat16)
        main = dot(dot(to_q_ref[...], values).astype(jnp.bfloat16), to_k_ref[...])
        ref[0:WIN_TOK, :] = main.astype(jnp.int32)
        rest = dot(dot(to_q_rest_ref[...], values).astype(jnp.bfloat16), to_k_rest_ref[...])
        rest = jnp.where(rest_lane == rest_row, rest, 0.0).astype(jnp.bfloat16)
        rest = dot(gather, rest).astype(jnp.int32)
        ref[WIN_TOK : WIN_TOK + 16, :] = rest[:, 0:128]
        ref[WIN_TOK + 16 : WIN_TOK + 32, :] = rest[:, 128:256]


def stack_tables(a, before_ref, own_ref, rows_ref, table_ref):
    positions = own_ref.shape[-1]
    heads = own_ref.shape[1]
    size = heads * WIN_Z
    edge = 2 - 2 * a
    for window in (edge, 1)[: 2 - a]:
        ref = before_ref if window == 0 else own_ref.at[window - 1]
        for k in range(table_ref.shape[1] // BLOCK):
            end = min(positions, (k + 1) * LOW)
            for h in range(heads):
                part = ref[h, :, k * LOW : end].astype(jnp.float32)
                if end < (k + 1) * LOW:
                    fill = jnp.zeros((WIN_Z, (k + 1) * LOW - end), jnp.float32)
                    part = jnp.concatenate([part, fill], axis=1)
                row = (k * heads + h) * WIN_Z
                rows_ref[window, row : row + WIN_Z, :] = part
    for k in range(table_ref.shape[1] // BLOCK):
        both = [rows_ref[window, k * size : (k + 1) * size] for window in (edge, 1)]
        block = jnp.concatenate(both, axis=0)
        table_ref[a, k * BLOCK : (k + 1) * BLOCK, :] = block.astype(jnp.bfloat16)


def look_up_bias(a, closed, pad_ref, geometry_ref, low_ref, high_ref, table_ref, bias_ref, pause, halfway):
    highs = table_ref.shape[1] // BLOCK
    lat_total = pad_ref.shape[0]
    odd_row = iota((8, LOW), 0) % 2 == 1
    low_iota = iota((LOW, LOW), 0)

    def look_up(tile, low, high):
        hot = jnp.where(low_iota == low, 1.0, 0.0).astype(jnp.bfloat16)
        found = dot(table_ref[a], hot)
        high = jnp.broadcast_to(high, (8, LOW))
        total = [found[8 * j : 8 * j + 8] for j in range(6)]
        for k in range(1, highs):
            here = high == k
            for j in range(6):
                row = k * BLOCK + 8 * j
                total[j] = jnp.where(here, found[row : row + 8], total[j])
        geometry = geometry_ref[tile]
        key_row, same_half, same_level = geometry[0:1], geometry[1:2], geometry[2:3]
        levels = jnp.where(odd_row, jnp.broadcast_to(same_level, (8, LOW)), 1)
        allowed = [levels, levels]
        usable = jnp.zeros((1, LOW), jnp.int32)
        for n in range(WIN_LAT):
            source = (lat_total - HALF_LAT + n) % lat_total
            usable = jnp.where(key_row == n, pad_ref[source], usable)
        usable = jnp.where(usable == 1, same_half, 0)
        usable = jnp.maximum(usable, 1 - closed)
        allowed[0] = levels * jnp.broadcast_to(usable, (8, LOW))
        return [
            jnp.where(allowed[s] == 1, total[s * 3 + kind] * LOG2E, SHUT)
            for s in range(2)
            for kind in range(3)
        ]

    def pair(p, carry):
        tile = a * 36 + p

        def two(ref):
            return jnp.concatenate(
                [ref[pl.ds(2 * tile, 1), :], ref[pl.ds(2 * tile + 1, 1), :]], axis=1
            )

        pieces = look_up(tile, two(low_ref), two(high_ref))
        for s in range(2):
            for kind in range(3):
                part = pieces[s * 3 + kind]
                bias_ref[a, s, kind, 2 * p, :, 0:128] = part[:, 0:128]
                bias_ref[a, s, kind, 2 * p + 1, :, 0:128] = part[:, 128:256]
        return carry

    lax.fori_loop(0, pause, pair, 0, unroll=6)
    halfway()
    lax.fori_loop(pause, 36, pair, 0, unroll=6)
    for tile in range(5):
        row = WIN_TOK + a * 5 + tile

        def wide(ref, row=row):
            return jnp.concatenate([ref[pl.ds(row, 1), :], ref[pl.ds(row + 16, 1), :]], axis=1)

        pieces = look_up(72 + a * 5 + tile, wide(low_ref), wide(high_ref))
        for j in range(16):
            q = tile * 16 + j
            if q < 72:
                for s in range(2):
                    for kind in range(3):
                        part = pieces[s * 3 + kind]
                        bias_ref[a, s, kind, q, :, 128:144] = part[:, 16 * j : 16 * j + 16]


def layer_kernel(*refs):
    inputs, refs = refs[:18], refs[18:]
    out_ref, refs = refs[0], refs[1:]
    copies, refs = refs[:18], refs[18:]
    (
        before_ref,
        hidden_ref,
        tokens_ref,
        from_lon_ref,
        from_lat_ref,
        queries_ref,
        keys_ref,
        tails_ref,
        low_ref,
        high_ref,
        rows_ref,
        table_ref,
        bias_ref,
        attended_ref,
        scores_ref,
        weights_ref,
        local_sem,
        send_sem,
        recv_sem,
        table_sem,
        lat_send_sem,
        lat_recv_sem,
    ) = refs
    lat = lax.axis_index("lat")
    lon = lax.axis_index("lon")
    lon_count = lax.axis_size("lon")
    other = 1 - lat
    left = lax.rem(lon + lon_count - 1, lon_count)
    right = lax.rem(lon + 1, lon_count)
    loads = [
        pltpu.make_async_copy(source, target, local_sem.at[n])
        for n, (source, target) in enumerate(zip(inputs, copies))
    ]
    for load in loads:
        load.start()
    (
        state_ref,
        land_mask_ref,
        land_embed_ref,
        pick_ref,
        w_qkv_ref,
        table_own_ref,
        index_ref,
        to_q_ref,
        to_k_ref,
        to_q_rest_ref,
        to_k_rest_ref,
        geometry_ref,
        pad_ref,
        w_proj_ref,
        offset_ref,
        gain_ref,
        shift_ref,
        restore_ref,
    ) = copies
    barrier = pltpu.get_barrier_semaphore()
    for device in ({"lon": left}, {"lon": right}, {"lat": other}):
        pl.semaphore_signal(barrier, inc=1, device_id=device, device_id_type=MESH)

    lat_rows, lon_columns, levels, features = state_ref.shape
    strip = lon_columns * levels
    part_rows = HALF_LAT * strip
    with jax.named_scope("wait_state"):
        for n in (1, 2, 0):
            loads[n].wait()

    def embed(i, carry):
        sea, land = (
            jnp.broadcast_to(land_embed_ref[n : n + 1, :], (levels, features)) for n in range(2)
        )
        rows = []
        for j in range(lon_columns):
            embedded = jnp.where(land_mask_ref[i, j] == 1, land, sea)
            rows.append(state_ref[i, j].astype(jnp.float32) + embedded)
        hidden = jnp.concatenate(rows, axis=0).astype(jnp.bfloat16).astype(jnp.float32)
        hidden_ref[pl.ds(pl.multiple_of(i * strip, strip), strip), :] = hidden
        return carry

    with jax.named_scope("embed"):
        lax.fori_loop(0, lat_rows, embed, 0)

    edge = 3 * other
    wrap = 3 * lat
    quarters = (edge, wrap, 1, 2)
    halves = (lat, other, 0, 1)
    loads[3].wait()

    def natural_rows(quarter):
        return pl.ds(pl.multiple_of(quarter * part_rows, 16), part_rows)

    def group(quarter):
        return dot(pick_ref[...], hidden_ref[natural_rows(quarter)].astype(jnp.bfloat16))

    def group_pair(n):
        first, second = group(quarters[2 * n]), group(quarters[2 * n + 1])
        for side in range(2):
            part = slice(side * PAIR, (side + 1) * PAIR)
            both = jnp.concatenate([first[part], second[part]], axis=0)
            tokens_ref[side, 2 * n * PAIR : 2 * (n + 1) * PAIR] = both.astype(jnp.bfloat16)

    pieces = ((0, 80), (144, 80), (224, 64), (80, 64))

    far = lax.rem(lon, 2)
    near = 1 - far

    def lon_copy(side, n):
        start, size = pieces[n]
        return pltpu.make_async_remote_copy(
            src_ref=tokens_ref.at[side, pl.ds(start, size)],
            dst_ref=from_lon_ref.at[1 - side, pl.ds(start, size)],
            send_sem=send_sem.at[side, n],
            recv_sem=recv_sem.at[1 - side, n],
            device_id={"lon": jnp.where(side == 1, right, left)},
            device_id_type=MESH,
        )

    def lat_copy(column):
        source = tokens_ref.at[column - 1] if column in (1, 2) else from_lon_ref.at[column // 3]
        return pltpu.make_async_remote_copy(
            src_ref=source.at[pl.ds(0, EDGE_ROWS)],
            dst_ref=from_lat_ref.at[column],
            send_sem=lat_send_sem.at[column],
            recv_sem=lat_recv_sem.at[column],
            device_id={"lat": other},
            device_id_type=MESH,
        )

    table_copy = pltpu.make_async_remote_copy(
        src_ref=table_own_ref.at[1],
        dst_ref=before_ref,
        send_sem=table_sem.at[0],
        recv_sem=table_sem.at[1],
        device_id={"lat": other},
        device_id_type=MESH,
    )

    with jax.named_scope("group0"):
        group_pair(0)
    with jax.named_scope("group1"):
        group_pair(1)

    def place(values, window, side, a, b):
        row = pl.multiple_of(32 * (2 * a + b), 32)
        for zw in range(2):
            part = values[32 * zw : 32 * zw + 32].astype(jnp.bfloat16)
            for n in range(6):
                keys_ref[window, side, n, pl.ds(row, 32), 128 * zw : 128 * zw + 128] = part[
                    :, 128 * n : 128 * n + 128
                ]
        tails_ref[window, side, 2 * a + b] = values[64:72]

    lower = iota((8, 2 * WIDTH), 0) < 4

    def place_tails(window, side):
        t = [tails_ref[window, side, n] for n in range(4)]
        for zw in range(2):
            rows = []
            for n in (0, 2):
                x, y = t[n], t[n + 1]
                if zw == 0:
                    y = pltpu.roll(y, 4, 0)
                else:
                    x = pltpu.roll(x, 4, 0)
                rows.append(jnp.where(lower, x, y))
            both = jnp.concatenate(rows, axis=0).astype(jnp.bfloat16)
            for n in range(6):
                keys_ref[window, side, n, 128:144, 128 * zw : 128 * zw + 128] = both[
                    :, 128 * n : 128 * n + 128
                ]

    loads[5].wait()
    with jax.named_scope("barrier"):
        pl.semaphore_wait(barrier, 3)
    lon_copy(far, 0).start()
    for n in range(4):
        lon_copy(near, n).start()
    table_copy.start()
    for column in (1, 2):
        lat_copy(column).start()

    for n in range(2):
        for g in range(3):
            scores_ref[n, g, :, 128:256] = jnp.full((8 * GROUP, 128), SHUT, jnp.float32)
    for side in range(2):
        empty = pl.multiple_of(64 * lat, 64)
        for n in range(6):
            keys_ref[1, side, n, pl.ds(empty, 64), :] = jnp.zeros((64, 256), jnp.bfloat16)
        for b in range(2):
            tails_ref[1, side, 2 * lat + b] = jnp.zeros((8, 2 * WIDTH), jnp.float32)

    with jax.named_scope("planes"):
        for n in range(6, 13):
            loads[n].wait()
        index_planes(
            index_ref, to_q_ref, to_k_ref, to_q_rest_ref, to_k_rest_ref, low_ref, high_ref
        )
    with jax.named_scope("qkv"):
        loads[4].wait()
        for side in range(2):
            for n in range(2):
                tokens = tokens_ref[side, 2 * n * PAIR : 2 * (n + 1) * PAIR]
                qkv = dot(tokens, w_qkv_ref[...])
                for m in range(2):
                    slot = 2 * n + m
                    part = qkv[m * PAIR : (m + 1) * PAIR]
                    queries = part[:, 0:WIDTH].astype(jnp.bfloat16).astype(jnp.float32)
                    for zw in range(2):
                        main = queries[32 * zw : 32 * zw + 32]
                        tail = queries[64 + 4 * zw : 68 + 4 * zw]
                        for g in range(3):
                            lanes = slice(128 * g, 128 * g + 128)
                            out = slice(128 * zw, 128 * zw + 128)
                            queries_ref[side, slot, g, 0:32, out] = main[:, lanes]
                            queries_ref[side, slot, g, 32:36, out] = tail[:, lanes]
                    place(part[:, WIDTH:], min(slot, 2), side, halves[slot], 1 - side)

    with jax.named_scope("stack"):
        stack_tables(0, before_ref, table_own_ref, rows_ref, table_ref)

    def bias(a, closed, pause, halfway):
        look_up_bias(
            a, closed, pad_ref, geometry_ref, low_ref, high_ref, table_ref, bias_ref, pause, halfway
        )

    def send_own():
        for n in (1, 2):
            lon_copy(far, n).start()

    def forward():
        for side in range(2):
            lon_copy(1 - side, 0).wait_recv()
        for column in (0, 3):
            lat_copy(column).start()

    def project(tokens):
        return dot(tokens, w_qkv_ref[:, WIDTH : 3 * WIDTH])

    head_mask = jnp.where(
        (iota((8, 256), 1) // 128 == iota((8, 256), 0) % 2)
        & (iota((8, 256), 1) % 128 // HEAD_DIM == iota((8, 256), 0) // 2),
        1.0,
        0.0,
    )
    gather_rows = jnp.where(
        iota((SLOT, 8 * GROUP), 1) // 8 == iota((SLOT, 8 * GROUP), 0), 1.0, 0.0
    ).astype(jnp.bfloat16)

    def place_of(step):
        kind, side = step // 2, lax.rem(step, 2)
        slot = jnp.where(kind == 0, 0, jnp.where(kind == 3, 1, kind + 1))
        return slot, side

    def score(step, g):
        slot, side = place_of(step)
        half = jnp.where(slot == 0, lat, jnp.where(slot == 1, other, slot - 2))
        edge_kind = jnp.where(slot < 2, 0, 1)
        window = jnp.minimum(slot, 2)
        first = pl.multiple_of((1 - side) * GROUP, GROUP)
        spread = jnp.concatenate(
            [
                jnp.broadcast_to(queries_ref[side, slot, g, t : t + 1], (8, 256)) * head_mask
                for t in range(GROUP)
            ],
            axis=0,
        )
        scores = lax.dot_general(
            spread.astype(jnp.bfloat16),
            keys_ref[window, side, g],
            (((1,), (1,)), ((), ())),
            preferred_element_type=jnp.float32,
        )
        bias = bias_ref[half, edge_kind, g, pl.ds(first, GROUP)].reshape(8 * GROUP, 256)
        scores_ref[lax.rem(step, 2), g, :, 0:WIN_TOK] = scores * SCALE + bias[:, 0:WIN_TOK]

    def weigh(step, g):
        scores = scores_ref[lax.rem(step, 2), g]
        powers = jnp.exp2(scores - jnp.max(scores, axis=-1, keepdims=True))
        inverse = 1.0 / jnp.sum(powers, axis=-1, keepdims=True)
        weights_ref[lax.rem(step, 2), g] = (powers * inverse).astype(jnp.bfloat16)

    def mix(step, g):
        slot, side = place_of(step)
        window = jnp.minimum(slot, 2)
        weights = weights_ref[lax.rem(step, 2), g, :, 0:WIN_TOK]
        mixed = dot(weights, keys_ref[window, side, 3 + g])
        mixed = (mixed.reshape(GROUP, 8, 256) * head_mask[None]).reshape(8 * GROUP, 256)
        part = dot(gather_rows, mixed.astype(jnp.bfloat16)).astype(jnp.bfloat16)
        for zw in range(2):
            row = pl.multiple_of((side * 2 + zw) * SLOT, SLOT)
            attended_ref[slot, pl.ds(row, SLOT), 128 * g : 128 * g + 128] = part[
                :, 128 * zw : 128 * zw + 128
            ]

    def stages(*parts):
        for g in range(3):
            for stage, step in parts:
                stage(step, g)

    offset, gain, shift = offset_ref, gain_ref, shift_ref

    def finish(slot):
        quarter = quarters[slot]
        natural = dot(restore_ref[...], attended_ref[slot]).astype(jnp.bfloat16)
        projected = dot(natural, w_proj_ref[...]) + offset[...][None, :]
        centered = projected - jnp.mean(projected, axis=-1, keepdims=True)
        spread = jnp.mean(centered * centered, axis=-1, keepdims=True)
        normed = centered * lax.rsqrt(spread + norm_epsilon) * gain[...][None, :]
        normed = normed + shift[...][None, :]
        result = hidden_ref[natural_rows(quarter)] + normed
        for n in range(HALF_LAT * lon_columns):
            i, j = divmod(n, lon_columns)
            part = result[n * levels : (n + 1) * levels]
            out_ref[quarter * HALF_LAT + i, j] = part.astype(jnp.bfloat16)

    with jax.named_scope("bias_edge"):
        bias(0, (other == 0).astype(jnp.int32), 36, send_own)
    with jax.named_scope("stack2"):
        table_copy.wait()
        stack_tables(1, before_ref, table_own_ref, rows_ref, table_ref)
    with jax.named_scope("bias_wrap"):
        bias(1, (other == 1).astype(jnp.int32), 18, forward)
    for n in range(13, 18):
        loads[n].wait()
    with jax.named_scope("keys_edge"):
        values = project(from_lon_ref[:, 0:EDGE_ROWS].reshape(2 * EDGE_ROWS, features))
        for side in range(2):
            place(values[EDGE_ROWS * side : EDGE_ROWS * (side + 1)], 0, side, lat, side)
        for column in range(4):
            lat_copy(column).wait_recv()
        values = project(from_lat_ref[...].reshape(4 * EDGE_ROWS, features))
        for column in range(4):
            part = values[EDGE_ROWS * column : EDGE_ROWS * (column + 1)]
            place(part, 0, column // 2, other, column % 2)
        for side in range(2):
            place_tails(0, side)
    with jax.named_scope("attend_edge"):
        stages((score, 0), (score, 1))
        stages((weigh, 0), (weigh, 1))
        stages((mix, 0), (mix, 1))
    lon_copy(far, 3).start()
    with jax.named_scope("finish_edge"):
        finish(0)
    with jax.named_scope("wait_own"):
        for n in (1, 2):
            for side in range(2):
                lon_copy(1 - side, n).wait_recv()
    with jax.named_scope("keys_own"):
        for side in range(2):
            values = project(from_lon_ref[side, 2 * PAIR : 4 * PAIR])
            for m in range(2):
                place(values[m * PAIR : (m + 1) * PAIR], 2, side, m, side)
            place_tails(2, side)
    with jax.named_scope("attend_own"):
        stages((score, 2), (score, 3))
        stages((weigh, 2), (weigh, 3))
        stages((mix, 2), (score, 4), (mix, 3), (score, 5))
        stages((weigh, 4), (weigh, 5))
        stages((mix, 4), (mix, 5))
    with jax.named_scope("finish_own"):
        finish(2)
        finish(3)
    with jax.named_scope("wait_wrap"):
        for side in range(2):
            lon_copy(1 - side, 3).wait_recv()
    with jax.named_scope("keys_wrap"):
        values = project(from_lon_ref[:, 64 : 2 * PAIR].reshape(2 * EDGE_ROWS, features))
        for side in range(2):
            start = EDGE_ROWS * side + 8
            place(values[start : start + PAIR], 1, side, other, side)
            place_tails(1, side)
    with jax.named_scope("attend_wrap"):
        stages((score, 6), (score, 7))
        stages((weigh, 6), (weigh, 7))
        stages((mix, 6), (mix, 7))
    with jax.named_scope("finish_wrap"):
        finish(1)
    with jax.named_scope("drain"):
        for side in range(2):
            for n in range(4):
                lon_copy(side, n).wait_send()
        for column in range(4):
            lat_copy(column).wait_send()


def as_tiles(rows):
    main = rows[:, :128].reshape(72, 256)
    rest = np.pad(rows[:, 128:].reshape(2, 72, 16), ((0, 0), (0, 8), (0, 0))).reshape(10, 256)
    return np.concatenate([main, rest], axis=0)


def bias_constants():
    queries, keys = window_orders()
    eye = np.eye(WIN_TOK, dtype=np.float32)
    to_q = eye[queries]
    to_q_rest = np.pad(to_q.reshape(2, 72, WIN_TOK), ((0, 0), (0, 8), (0, 0)))
    to_q_rest = to_q_rest.reshape(160, WIN_TOK)
    to_k = eye[keys[:128]].T
    to_k_rest = eye[np.tile(keys[128:], 16)].T
    q_level, q_half = queries // 72, queries // 12 % 6 // 3
    k_level, k_row = keys // 72, keys // 12 % 6
    planes = [
        np.broadcast_to(k_row[None, :], (WIN_TOK, WIN_TOK)),
        q_half[:, None] == (k_row // 3)[None, :],
        q_level[:, None] == k_level[None, :],
    ]
    geometry = np.stack([as_tiles(p.astype(np.int32)) for p in planes], axis=1)
    matrices = [jnp.asarray(m, jnp.bfloat16) for m in (to_q, to_k, to_q_rest, to_k_rest)]
    return matrices + [jnp.asarray(geometry)]


def group_constants(levels, columns):
    rows = HALF_LAT * columns * levels
    pick = np.zeros((2 * PAIR, rows), np.float32)
    restore = np.zeros((rows, 2 * WIN_Z * SLOT), np.float32)
    for side in range(2):
        for zw in range(WIN_Z):
            for t in range(GROUP):
                dz, rest = divmod(t, HALF_LAT * HALF_LON)
                di, dj = divmod(rest, HALF_LON)
                z = (WIN_Z * zw + dz + WIN_Z // 2) % levels
                natural = (di * columns + side * HALF_LON + dj) * levels + z
                place = 32 * zw + t if t < 32 else 64 + 4 * zw + t - 32
                pick[side * PAIR + place, natural] = 1.0
                restore[natural, (side * WIN_Z + zw) * SLOT + t] = 1.0
    return jnp.asarray(pick, jnp.bfloat16), jnp.asarray(restore, jnp.bfloat16)


def on_device(
    state_tokens,
    land_mask,
    pad_mask,
    land_embed,
    w_qkv,
    w_proj,
    proj_bias,
    norm_gain,
    norm_shift,
    bias_table,
    index_table,
):
    levels, lat_rows, lon_columns, features = state_tokens.shape
    assert (levels, lat_rows, lon_columns) == (2 * WIN_Z, 2 * WIN_LAT, WIN_LON)
    assert lax.axis_size("lat") == 2 and lax.axis_size("lon") > 2
    highs = -(-bias_table.shape[-1] // LOW)
    pick, restore = group_constants(levels, lon_columns)
    to_q, to_k, to_q_rest, to_k_rest, geometry = bias_constants()
    state = state_tokens.transpose(1, 2, 0, 3)
    table = bias_table.transpose(0, 2, 1, 3)
    inputs = [
        state,
        land_mask,
        land_embed,
        pick,
        w_qkv,
        table,
        index_table,
        to_q,
        to_k,
        to_q_rest,
        to_k_rest,
        geometry,
        pad_mask,
        w_proj,
        proj_bias,
        norm_gain,
        norm_shift,
        restore,
    ]
    bf16, f32, i32 = jnp.bfloat16, jnp.float32, jnp.int32
    dma = pltpu.SemaphoreType.DMA
    scalars = (1, 12)
    copies = [
        (pltpu.SMEM if n in scalars else pltpu.VMEM)(x.shape, x.dtype)
        for n, x in enumerate(inputs)
    ]
    tokens = levels * lat_rows * lon_columns
    out = pl.pallas_call(
        layer_kernel,
        out_shape=pltpu.VMEM(state.shape, bf16),
        in_specs=[pl.BlockSpec(memory_space=pltpu.HBM)] * len(inputs),
        out_specs=pl.BlockSpec(memory_space=pltpu.VMEM),
        scratch_shapes=copies
        + [
            pltpu.VMEM(table.shape[1:], bf16),
            pltpu.VMEM((tokens, features), f32),
            pltpu.VMEM((2, 4 * PAIR, features), bf16),
            pltpu.VMEM((2, 4 * PAIR, features), bf16),
            pltpu.VMEM((4, EDGE_ROWS, features), bf16),
            pltpu.VMEM((2, 4, 3, 40, 256), f32),
            pltpu.VMEM((3, 2, 6, WIN_TOK, 256), bf16),
            pltpu.VMEM((3, 2, 4, 8, 2 * WIDTH), f32),
            pltpu.VMEM((WIN_TOK + 32, 128), i32),
            pltpu.VMEM((WIN_TOK + 32, 128), i32),
            pltpu.VMEM((3, highs * BLOCK // 2, LOW), f32),
            pltpu.VMEM((2, highs * BLOCK, LOW), bf16),
            pltpu.VMEM((2, 2, 3, 2 * GROUP, 8, 256), f32),
            pltpu.VMEM((4, 4 * SLOT, WIDTH), bf16),
            pltpu.VMEM((2, 3, 8 * GROUP, 256), f32),
            pltpu.VMEM((2, 3, 8 * GROUP, 256), bf16),
            dma((len(inputs),)),
            dma((2, 4)),
            dma((2, 4)),
            dma((2,)),
            dma((4,)),
            dma((4,)),
        ],
        compiler_params=pltpu.CompilerParams(
            collective_id=0, has_side_effects=True, vmem_limit_bytes=56 << 20
        ),
        name="layer",
    )(*inputs)
    return out.transpose(2, 0, 1, 3)


def solution(mesh):
    in_specs = (
        P("member", "lat", "lon", None),
        P("lat", "lon"),
        P(),
        P(),
        P(),
        P(),
        P(),
        P(),
        P(),
        P("lat", None, None, None),
        P(),
    )
    out_specs = P("member", "lat", "lon", None)
    return jax.shard_map(
        on_device, mesh=mesh, in_specs=in_specs, out_specs=out_specs, check_vma=False
    )
```
